32 devices in a mesh: dp: 4 (over y, z), sp: 8 (over x, core).
Axes of the slice: x: 4, y: 2, z: 2, core: 2. Of those that a mesh axis runs over, the one named last changes fastest.
The devices are a block of a 4x4x8 slice.
Arguments:
- x_in: bfloat16 [8, 2048, 2304], P('dp', 'sp'), parts along dimension 0
- dy_in: bfloat16 [8, 2048, 2304], P('dp', 'sp'), parts along dimension 0
- positions: int32 [8192], P(('dp', 'sp')), parts along dimension 0
- w_q: bfloat16 [2304, 2048], replicated
- w_k: bfloat16 [2304, 1024], replicated
- w_v: bfloat16 [2304, 1024], replicated
- w_o: bfloat16 [2048, 2304], replicated
- w_pre: float32 [2304], replicated
- w_post: float32 [2304], replicated
- q_norm: float32 [256], replicated
- k_norm: float32 [256], replicated
Outputs:
- output 1: bfloat16 [8, 2048, 2304], P('dp', 'sp'), parts along dimension 0
- output 2: bfloat16 [8, 2048, 2304], P('dp', 'sp'), parts along dimension 0
- output 3: bfloat16 [9216, 2048], P('dp'), parts along dimension 0
- output 4: bfloat16 [9216, 1024], P('dp'), parts along dimension 0
- output 5: bfloat16 [9216, 1024], P('dp'), parts along dimension 0
- output 6: bfloat16 [8192, 2304], P('dp'), parts along dimension 0
- output 7: float32 [9216], P('dp'), parts along dimension 0
- output 8: float32 [9216], P('dp'), parts along dimension 0
- output 9: float32 [1024], P('dp'), parts along dimension 0
- output 10: float32 [1024], P('dp'), parts along dimension 0
There are 4 independent parts. The reference program is written for one: setup_inputs(seed, part) draws one part's arguments, and reference() takes and returns one part's arrays. A program takes and returns all parts, laid end to end along the dimension named above; an argument that names none is the same for every part.
All inputs are finite; a program needn't handle non-finite values.
Results may differ from the reference program's by a relative error of at most 0.02.
Values are sent between devices in bfloat16 or wider.
A program may use at most 768 MiB of HBM per device.

```python
import functools
import jax
import jax.numpy as jnp
from jax import lax

B = 2
SEQ = 2048
D = 2304
H = 8
K = 4
HEAD = 256

EPS = 1e-6
ROPE_BASE = 1000000.0
ROPE_SCALE = 8.0
NEG_BIG = -1e30
Q_ROWS = min(128, SEQ)


def setup_inputs(seed: int = 0, part: int = 0) -> dict:
    base_key = jax.random.key(seed)
    own = jax.random.split(jax.random.fold_in(base_key, part), 4)
    shared = jax.random.split(base_key, 8)
    x_in = jax.random.normal(own[0], (B, SEQ, D), jnp.float32).astype(jnp.bfloat16)
    dy_in = jax.random.normal(own[1], (B, SEQ, D), jnp.float32).astype(jnp.bfloat16)
    start = jax.random.randint(own[2], (1,), 0, 1000)
    gaps = jax.random.randint(own[3], (SEQ,), 1, 5)
    positions = (start + jnp.cumsum(gaps) - gaps[0]).astype(jnp.int32)
    w_q = (jax.random.normal(shared[0], (D, H * HEAD), jnp.float32) * D ** -0.5).astype(jnp.bfloat16)
    w_k = (jax.random.normal(shared[1], (D, K * HEAD), jnp.float32) * D ** -0.5).astype(jnp.bfloat16)
    w_v = (jax.random.normal(shared[2], (D, K * HEAD), jnp.float32) * D ** -0.5).astype(jnp.bfloat16)
    w_o = (jax.random.normal(shared[3], (H * HEAD, D), jnp.float32) * (H * HEAD) ** -0.5).astype(jnp.bfloat16)
    w_pre = 0.3 * jax.random.normal(shared[4], (D,), jnp.float32)
    w_post = 0.3 * jax.random.normal(shared[5], (D,), jnp.float32)
    q_norm = 0.3 + 0.3 * jax.random.normal(shared[6], (HEAD,), jnp.float32)
    k_norm = 0.3 + 0.3 * jax.random.normal(shared[7], (HEAD,), jnp.float32)
    return {'x_in': x_in, 'dy_in': dy_in, 'positions': positions, 'w_q': w_q, 'w_k': w_k, 'w_v': w_v, 'w_o': w_o, 'w_pre': w_pre, 'w_post': w_post, 'q_norm': q_norm, 'k_norm': k_norm}


def rms_scale(x_f32, weight):
    inv_rms = lax.rsqrt(jnp.mean(x_f32 * x_f32, axis=-1, keepdims=True) + EPS)
    return x_f32 * inv_rms * (1.0 + weight)


def norm_rope(heads_f32, weight, cosines, sines):
    half_dim = HEAD // 2
    normed = rms_scale(heads_f32, weight)
    first = normed[..., :half_dim]
    second = normed[..., half_dim:]
    cos_b = cosines[None, :, None, :]
    sin_b = sines[None, :, None, :]
    return jnp.concatenate([first * cos_b - second * sin_b, second * cos_b + first * sin_b], axis=-1)


def attention(q_rot, k_rot, v_heads):
    group = H // K
    blocks = SEQ // Q_ROWS
    q_blocks = jnp.moveaxis(q_rot.reshape(B, blocks, Q_ROWS, K, group, HEAD), 1, 0)
    key_f32 = k_rot.astype(jnp.float32)
    val_f32 = v_heads.astype(jnp.float32)
    col_ids = jnp.arange(SEQ)

    def one_block(item):
        q_blk, index = item
        scores = jnp.einsum('bqkgh,bskh->bkgqs', q_blk.astype(jnp.float32), key_f32) * HEAD ** -0.5
        row_ids = index * Q_ROWS + jnp.arange(Q_ROWS)
        scores = jnp.where(row_ids[:, None] >= col_ids[None, :], scores, NEG_BIG)
        attn_prob = jax.nn.softmax(scores, axis=-1).astype(jnp.bfloat16).astype(jnp.float32)
        return jnp.einsum('bkgqs,bskh->bqkgh', attn_prob, val_f32).astype(jnp.bfloat16)

    block_out = lax.map(jax.checkpoint(one_block), (q_blocks, jnp.arange(blocks)))
    return jnp.moveaxis(block_out, 0, 1).reshape(B, SEQ, H, HEAD)


def forward(positions, x_in, w_q, w_k, w_v, w_o, w_pre, w_post, q_norm, k_norm):
    x_f32 = x_in.astype(jnp.float32)
    normed = rms_scale(x_f32, w_pre).astype(jnp.bfloat16).astype(jnp.float32)
    q_proj = jnp.einsum('bsd,dn->bsn', normed, w_q.astype(jnp.float32)).astype(jnp.bfloat16)
    k_proj = jnp.einsum('bsd,dn->bsn', normed, w_k.astype(jnp.float32)).astype(jnp.bfloat16)
    v_proj = jnp.einsum('bsd,dn->bsn', normed, w_v.astype(jnp.float32)).astype(jnp.bfloat16)
    half_dim = HEAD // 2
    inv_freq = ROPE_BASE ** (-jnp.arange(half_dim, dtype=jnp.float32) * 2.0 / HEAD)
    angles = (positions.astype(jnp.float32) / ROPE_SCALE)[:, None] * inv_freq[None, :]
    cosines = jnp.cos(angles)
    sines = jnp.sin(angles)
    q_rot = norm_rope(q_proj.reshape(B, SEQ, H, HEAD).astype(jnp.float32), q_norm, cosines, sines).astype(jnp.bfloat16)
    k_rot = norm_rope(k_proj.reshape(B, SEQ, K, HEAD).astype(jnp.float32), k_norm, cosines, sines).astype(jnp.bfloat16)
    v_heads = v_proj.reshape(B, SEQ, K, HEAD)
    attn_out = attention(q_rot, k_rot, v_heads)
    proj = jnp.einsum('bsn,nd->bsd', attn_out.reshape(B, SEQ, H * HEAD).astype(jnp.float32), w_o.astype(jnp.float32)).astype(jnp.bfloat16)
    return (x_f32 + rms_scale(proj.astype(jnp.float32), w_post)).astype(jnp.bfloat16)


def reference(x_in, dy_in, positions, w_q, w_k, w_v, w_o, w_pre, w_post, q_norm, k_norm):
    y_out, pullback = jax.vjp(functools.partial(forward, positions), x_in, w_q, w_k, w_v, w_o, w_pre, w_post, q_norm, k_norm)
    grads = pullback(dy_in)
    return (y_out, grads[0], grads[1], grads[2], grads[3], grads[4], grads[5], grads[6], grads[7], grads[8])
```

```python
import functools
import jax
import jax.numpy as jnp
from jax import lax
from jax.experimental import pallas as pl
from jax.experimental.pallas import tpu as pltpu
from jax.sharding import PartitionSpec as P

EPS = 1e-6
ROPE_BASE = 1000000.0
ROPE_SCALE = 8.0
NEG_BIG = -1e30
BLK = 256
BF = jnp.bfloat16
F32 = jnp.float32


def rms_scale(x_f32, weight):
    inv_rms = lax.rsqrt(jnp.mean(x_f32 * x_f32, axis=-1, keepdims=True) + EPS)
    return x_f32 * inv_rms * (1.0 + weight)


def pre_norm(x_f32, weight):
    return rms_scale(x_f32, weight).astype(BF)


def post_norm(proj, weight):
    return rms_scale(proj.astype(F32), weight)


def rope_tables(positions, head):
    half_dim = head // 2
    inv_freq = ROPE_BASE ** (-jnp.arange(half_dim, dtype=F32) * 2.0 / head)
    angles = (positions.astype(F32) / ROPE_SCALE)[:, None] * inv_freq[None, :]
    return jnp.cos(angles), jnp.sin(angles)


def norm_rope(head_bf, weight, cosines, sines):
    half_dim = head_bf.shape[-1] // 2
    normed = rms_scale(head_bf.astype(F32), weight)
    first = normed[..., :half_dim]
    second = normed[..., half_dim:]
    rotated = jnp.concatenate([first * cosines - second * sines, second * cosines + first * sines], axis=-1)
    return rotated.astype(BF)


def nt(lhs, rhs):
    return lax.dot_general(lhs, rhs, (((1,), (1,)), ((), ())), preferred_element_type=F32)


def nn(lhs, rhs):
    return lax.dot_general(lhs, rhs, (((1,), (0,)), ((), ())), preferred_element_type=F32)


def tn(lhs, rhs):
    return lax.dot_general(lhs, rhs, (((0,), (0,)), ((), ())), preferred_element_type=F32)


def fwd_kernel(q_ref, k_ref, v_ref, o_ref, lse_ref, s_scr, acc):
    seq, head = q_ref.shape
    scale = head ** -0.5
    lower = lax.broadcasted_iota(jnp.int32, (BLK, BLK), 0) >= lax.broadcasted_iota(jnp.int32, (BLK, BLK), 1)

    def fold(x, op):
        out = x[:, :128]
        for c in range(1, x.shape[1] // 128):
            out = op(out, x[:, c * 128:(c + 1) * 128])
        return out

    @pl.loop(0, seq // BLK)
    def _(i):
        rows = pl.ds(pl.multiple_of(i * BLK, BLK), BLK)
        q = q_ref[rows, :]
        s = jnp.where(lower, nt(q, k_ref[rows, :]) * scale, NEG_BIG)
        s_scr[:, rows] = s

        def pass1(j, m):
            cols = pl.ds(pl.multiple_of(j * BLK, BLK), BLK)
            s = nt(q, k_ref[cols, :]) * scale
            s_scr[:, cols] = s
            return jnp.maximum(m, fold(s, jnp.maximum))

        m = lax.fori_loop(0, i, pass1, fold(s, jnp.maximum))
        m = jnp.max(m, axis=1, keepdims=True)

        def pass2(j, l):
            cols = pl.ds(pl.multiple_of(j * BLK, BLK), BLK)
            p = jnp.exp(s_scr[:, cols] - m)
            s_scr[:, cols] = p
            return l + fold(p, jnp.add)

        l = lax.fori_loop(0, i + 1, pass2, jnp.zeros((BLK, 128), F32))
        l = jnp.sum(l, axis=1, keepdims=True)
        inv = 1.0 / l
        acc[...] = jnp.zeros_like(acc)

        @pl.loop(0, i + 1)
        def _(j):
            cols = pl.ds(pl.multiple_of(j * BLK, BLK), BLK)
            acc[...] += nn((s_scr[:, cols] * inv).astype(BF), v_ref[cols, :])

        o_ref[rows, :] = acc[...].astype(BF)
        lse_ref[rows, :] = m + jnp.log(l)


def attn_fwd(q, k, v):
    seq, head = q.shape
    pairs = seq * (seq + BLK) // 2
    return pl.pallas_call(
        fwd_kernel,
        out_shape=(jax.ShapeDtypeStruct((seq, head), BF), jax.ShapeDtypeStruct((seq, 1), F32)),
        in_specs=[pl.BlockSpec(memory_space=pltpu.VMEM)] * 3,
        out_specs=(pl.BlockSpec(memory_space=pltpu.VMEM),) * 2,
        scratch_shapes=[pltpu.VMEM((BLK, seq), F32), pltpu.VMEM((BLK, head), F32)],
        cost_estimate=pl.CostEstimate(flops=4 * pairs * head, bytes_accessed=8 * seq * head, transcendentals=pairs),
        compiler_params=pltpu.CompilerParams(vmem_limit_bytes=32 * 1024 * 1024),
        name='attn_fwd',
    )(q, k, v)


def bwd_kernel(q_ref, k_ref, v_ref, do_ref, lse_ref, dl_ref, dq_ref, dk_ref, dv_ref, dq_acc):
    seq, head = q_ref.shape
    scale = head ** -0.5
    upper = lax.broadcasted_iota(jnp.int32, (BLK, BLK), 0) <= lax.broadcasted_iota(jnp.int32, (BLK, BLK), 1)
    dq_acc[...] = jnp.zeros_like(dq_acc)
    dk_ref[...] = jnp.zeros_like(dk_ref)
    dv_ref[...] = jnp.zeros_like(dv_ref)

    @pl.loop(0, seq // BLK)
    def _(j):
        cols = pl.ds(pl.multiple_of(j * BLK, BLK), BLK)
        k = k_ref[cols, :]
        v = v_ref[cols, :]

        def step(i, masked):
            rows = pl.ds(pl.multiple_of(i * BLK, BLK), BLK)
            q = q_ref[rows, :]
            do = do_ref[rows, :]
            st = nt(k, q) * scale
            if masked:
                st = jnp.where(upper, st, NEG_BIG)
            pt = jnp.exp(st - lse_ref[0:1, rows])
            dpt = nt(v, do)
            dst = (pt * (dpt - dl_ref[0:1, rows]) * scale).astype(BF)
            dv_ref[cols, :] += nn(pt.astype(BF), do)
            dk_ref[cols, :] += nn(dst, q)
            dq_acc[rows, :] += tn(dst, k)

        step(j, True)

        @pl.loop(j + 1, seq // BLK)
        def _(i):
            step(i, False)

    dq_ref[...] = dq_acc[...].astype(BF)


def attn_bwd(q, k, v, do, lse, delta):
    seq, head = q.shape
    pairs = seq * (seq + BLK) // 2
    return pl.pallas_call(
        bwd_kernel,
        out_shape=(jax.ShapeDtypeStruct((seq, head), BF), jax.ShapeDtypeStruct((seq, head), F32), jax.ShapeDtypeStruct((seq, head), F32)),
        in_specs=[pl.BlockSpec(memory_space=pltpu.VMEM)] * 6,
        out_specs=(pl.BlockSpec(memory_space=pltpu.VMEM),) * 3,
        scratch_shapes=[pltpu.VMEM((seq, head), F32)],
        cost_estimate=pl.CostEstimate(flops=10 * pairs * head, bytes_accessed=20 * seq * head, transcendentals=pairs),
        compiler_params=pltpu.CompilerParams(vmem_limit_bytes=32 * 1024 * 1024),
        name='attn_bwd',
    )(q, k, v, do, lse, delta)


def solution(mesh):
    group = mesh.shape['sp']

    def device_step(x_in, dy_in, positions, w_q, w_k, w_v, w_o, w_pre, w_post, q_norm, k_norm):
        batch, seq_loc, width = x_in.shape
        head = q_norm.shape[0]
        heads = w_q.shape[1] // head
        kv_heads = w_k.shape[1] // head
        rep = group // kv_heads
        assert heads == group and rep == 2
        me = lax.axis_index('sp')
        kv = me // rep
        even = (me % rep) == 0
        swap = [(d, d ^ 1) for d in range(group)]

        def cols(w, index):
            return lax.dynamic_slice(w, (0, index * head), (w.shape[0], head))

        w_qkv = jnp.concatenate([cols(w_q, me), cols(w_k, kv), cols(w_v, kv)], axis=1)
        wo_mine = lax.dynamic_slice(w_o, (me * head, 0), (head, width))

        x_f32 = [x_in[b].astype(F32) for b in range(batch)]
        dy_f32 = [dy_in[b].astype(F32) for b in range(batch)]
        a_all, pre_pulls = [], []
        for b in range(batch):
            normed, pull = jax.vjp(pre_norm, x_f32[b], w_pre)
            pre_pulls.append(pull)
            a_all.append(lax.all_gather(normed, 'sp', axis=0, tiled=True))
        pos_all = lax.all_gather(positions, 'sp', axis=0, tiled=True)
        cosines, sines = rope_tables(pos_all, head)
        roper = functools.partial(norm_rope, cosines=cosines, sines=sines)

        saved = []
        dproj_all = []
        y_out, dw_post = [], 0.0
        for b in range(batch):
            qkv = nn(a_all[b], w_qkv).astype(BF)
            q_rot, q_pull = jax.vjp(roper, qkv[:, :head], q_norm)
            k_rot, k_pull = jax.vjp(roper, qkv[:, head:2 * head], k_norm)
            v_raw = qkv[:, 2 * head:]
            o, lse = attn_fwd(q_rot, k_rot, v_raw)
            saved.append((q_rot, k_rot, v_raw, o, lse, q_pull, k_pull))
            o_tok = lax.all_to_all(o, 'sp', 0, 1, tiled=True)
            proj = nn(o_tok, w_o).astype(BF)
            post, post_pull = jax.vjp(post_norm, proj, w_post)
            y_out.append((x_f32[b] + post).astype(BF))
            d_proj, dwp = post_pull(dy_f32[b])
            dw_post = dw_post + dwp
            dproj_all.append(lax.all_gather(d_proj, 'sp', axis=0, tiled=True))

        d_mine, dqkv_tok = [], []
        dq_norm = dk_norm = 0.0
        for b in range(batch):
            q_rot, k_rot, v_raw, o, lse, q_pull, k_pull = saved[b]
            d_o = nt(dproj_all[b], wo_mine).astype(BF)
            delta = jnp.sum(d_o.astype(F32) * o.astype(F32), axis=1)[None, :]
            dq_rot, dk_part, dv_part = attn_bwd(q_rot, k_rot, v_raw, d_o, lse.reshape(1, -1), delta)
            other = lax.ppermute(jnp.where(even, dv_part, dk_part), 'sp', swap)
            dkv = (jnp.where(even, dk_part, dv_part) + other).astype(BF)
            dq_proj, dqn = q_pull(dq_rot)
            dk_proj, dkn = k_pull(dkv)
            dq_norm = dq_norm + dqn
            dk_norm = dk_norm + jnp.where(even, dkn, 0.0)
            d_two = jnp.concatenate([dq_proj, jnp.where(even, dk_proj, dkv)], axis=1)
            d_mine.append(d_two)
            dqkv_tok.append(lax.all_to_all(d_two, 'sp', 0, 1, tiled=True))

        dw_o = sum(tn(saved[b][3], dproj_all[b]) for b in range(batch)).astype(BF)
        dw_o_all = lax.all_gather(dw_o, 'sp', axis=0, tiled=True)
        dw_two = sum(tn(a_all[b], d_mine[b]) for b in range(batch)).astype(BF)
        dw_all = lax.all_gather(dw_two, 'sp', axis=0, tiled=False)
        dw_all = dw_all.reshape(group, width, 2, head)
        dw_q_all = dw_all[:, :, 0].transpose(1, 0, 2).reshape(width, heads * head)
        dw_kv = dw_all[:, :, 1].reshape(kv_heads, rep, width, head)
        dw_k_all = dw_kv[:, 0].transpose(1, 0, 2).reshape(width, kv_heads * head)
        dw_v_all = dw_kv[:, 1].transpose(1, 0, 2).reshape(width, kv_heads * head)

        dx_out, dw_pre = [], 0.0
        for b in range(batch):
            d_tok = dqkv_tok[b].reshape(seq_loc, group, 2, head)
            dq_flat = d_tok[:, :, 0].reshape(seq_loc, heads * head)
            dkv_tok = d_tok[:, :, 1].reshape(seq_loc, kv_heads, rep, head)
            dk_flat = dkv_tok[:, :, 0].reshape(seq_loc, kv_heads * head)
            dv_flat = dkv_tok[:, :, 1].reshape(seq_loc, kv_heads * head)
            d_normed = (nt(dq_flat, w_q) + nt(dk_flat, w_k) + nt(dv_flat, w_v)).astype(BF)
            dx_norm, dwp = pre_pulls[b](d_normed)
            dw_pre = dw_pre + dwp
            dx_out.append((dy_f32[b] + dx_norm).astype(BF))
        small = lax.psum((dw_pre, dw_post, dq_norm, dk_norm), 'sp')
        return (jnp.stack(y_out), jnp.stack(dx_out), dw_q_all, dw_k_all, dw_v_all, dw_o_all) + small

    token_spec = P('dp', 'sp', None)
    return jax.shard_map(device_step, mesh=mesh,
                         in_specs=(token_spec, token_spec, P(('dp', 'sp')), P(None, None), P(None, None), P(None, None), P(None, None), P(None), P(None), P(None), P(None)),
                         out_specs=(token_spec, token_spec, P('dp', None), P('dp', None), P('dp', None), P('dp', None), P('dp'), P('dp'), P('dp'), P('dp')),
                         check_vma=False)
```

```python
import functools
import math
import jax
import jax.numpy as jnp
from jax import lax
from jax.experimental import pallas as pl
from jax.experimental.pallas import tpu as pltpu
from jax.sharding import PartitionSpec as P

EPS = 1e-6
ROPE_BASE = 1000000.0
ROPE_SCALE = 8.0
NEG_BIG = -1e30
HALF_PI = (1.5625, 0.0081787109375, 0.00011730194091796875, 3.129243850708008e-07, 9.920935796805404e-10)
BWD_BLK = 256
BF = jnp.bfloat16
F32 = jnp.float32
MESH = pl.DeviceIdType.MESH


def rms_scale(x_f32, weight):
    inv_rms = lax.rsqrt(jnp.mean(x_f32 * x_f32, axis=-1, keepdims=True) + EPS)
    return x_f32 * inv_rms * (1.0 + weight)


def pre_norm(x_f32, weight):
    return rms_scale(x_f32, weight).astype(BF)


def post_norm(proj, weight):
    return rms_scale(proj.astype(F32), weight)


def norm_rope(head_bf, weight, cosines, sines):
    half_dim = head_bf.shape[-1] // 2
    normed = rms_scale(head_bf.astype(F32), weight)
    first = normed[..., :half_dim]
    second = normed[..., half_dim:]
    rotated = jnp.concatenate([first * cosines - second * sines, second * cosines + first * sines], axis=-1)
    return rotated.astype(BF)


def nt(lhs, rhs):
    return lax.dot_general(lhs, rhs, (((1,), (1,)), ((), ())), preferred_element_type=F32)


def nn(lhs, rhs):
    return lax.dot_general(lhs, rhs, (((1,), (0,)), ((), ())), preferred_element_type=F32)


def tn(lhs, rhs):
    return lax.dot_general(lhs, rhs, (((0,), (0,)), ((), ())), preferred_element_type=F32)


def others_barrier(group, me):
    barrier = pltpu.get_barrier_semaphore()
    for step in range(1, group):
        pl.semaphore_signal(barrier, inc=1, device_id={'sp': lax.rem(me + step, group)}, device_id_type=MESH)
    pl.semaphore_wait(barrier, group - 1)


def block_of(index, size):
    return pl.ds(pl.multiple_of(index * size, size), size)


def fold(x, op):
    out = x[:, :128]
    for c in range(1, x.shape[1] // 128):
        out = op(out, x[:, c * 128:(c + 1) * 128])
    return out


class Attention:
    def __init__(self, group, me, q_ref, k_ref, v_ref, o_ref, lse_ref, tok_ref, s_scr, acc, send_sem, recv_sem):
        self.group, self.me = group, me
        self.refs = q_ref, k_ref, v_ref, o_ref, lse_ref, tok_ref, s_scr, acc
        self.sems = send_sem, recv_sem
        self.blk, self.head = acc.shape
        self.mine = block_of(me, self.head)

    def copy_to(self, step):
        o_ref, tok_ref = self.refs[3], self.refs[5]
        peer = lax.rem(self.me + step, self.group)
        return pltpu.make_async_remote_copy(
            src_ref=o_ref.at[block_of(peer, self.blk), :],
            dst_ref=tok_ref.at[:, self.mine],
            send_sem=self.sems[0].at[step],
            recv_sem=self.sems[1].at[step],
            device_id={'sp': peer},
            device_id_type=MESH,
        )

    def blocks(self, first, last):
        q_ref, k_ref, v_ref, o_ref, lse_ref, _, s_scr, acc = self.refs
        blk, head = self.blk, self.head
        scale = head ** -0.5
        lower = lax.broadcasted_iota(jnp.int32, (blk, blk), 0) >= lax.broadcasted_iota(jnp.int32, (blk, blk), 1)

        @pl.loop(first, last)
        def _(step):
            i = lax.rem(self.me + step, self.group)
            rows = block_of(i, blk)
            q = q_ref[rows, :]
            s = jnp.where(lower, nt(q, k_ref[rows, :]) * scale, NEG_BIG)
            s_scr[:, rows] = s

            def pass1(j, m):
                cols = block_of(j, blk)
                s = nt(q, k_ref[cols, :]) * scale
                s_scr[:, cols] = s
                return jnp.maximum(m, fold(s, jnp.maximum))

            m = lax.fori_loop(0, i, pass1, fold(s, jnp.maximum))
            m = jnp.max(m, axis=1, keepdims=True)

            @pl.when(step > 1)
            def _():
                self.copy_to(step - 1).start()

            def pass2(j, l):
                cols = block_of(j, blk)
                p = jnp.exp(s_scr[:, cols] - m)
                s_scr[:, cols] = p
                return l + fold(p, jnp.add)

            l = lax.fori_loop(0, i + 1, pass2, jnp.zeros((blk, min(128, blk)), F32))
            l = jnp.sum(l, axis=1, keepdims=True)
            inv = 1.0 / l
            acc[...] = jnp.zeros_like(acc)

            @pl.loop(0, i + 1)
            def _(j):
                cols = block_of(j, blk)
                acc[...] += nn((s_scr[:, cols] * inv).astype(BF), v_ref[cols, :])

            o_ref[rows, :] = acc[...].astype(BF)
            lse_ref[rows, :] = m + jnp.log(l)

    def flush(self):
        o_ref, tok_ref = self.refs[3], self.refs[5]
        tok_ref[:, self.mine] = o_ref[block_of(self.me, self.blk), :]
        self.copy_to(self.group - 1).start()

    def finish(self):
        @pl.loop(1, self.group)
        def _(step):
            self.copy_to(step).wait()


def fwd_kernel(group, *refs):
    me = lax.axis_index('sp')
    others_barrier(group, me)
    attention = Attention(group, me, *refs)
    attention.blocks(0, group)
    attention.flush()
    attention.finish()


def attn_scratch(group, blk, seq, head):
    return [pltpu.VMEM((blk, seq), F32), pltpu.VMEM((blk, head), F32), pltpu.SemaphoreType.DMA((group,)), pltpu.SemaphoreType.DMA((group,))]


def attn_outs(group, blk, seq, head):
    return jax.ShapeDtypeStruct((seq, head), BF), jax.ShapeDtypeStruct((seq, 1), F32), jax.ShapeDtypeStruct((blk, group * head), BF)


def attn_fwd(q, k, v, group, cid):
    seq, head = q.shape
    blk = seq // group
    pairs = seq * (seq + blk) // 2
    return pl.pallas_call(
        functools.partial(fwd_kernel, group),
        out_shape=attn_outs(group, blk, seq, head),
        in_specs=[pl.BlockSpec(memory_space=pltpu.VMEM)] * 3,
        out_specs=(pl.BlockSpec(memory_space=pltpu.VMEM),) * 3,
        scratch_shapes=attn_scratch(group, blk, seq, head),
        cost_estimate=pl.CostEstimate(flops=24 * pairs * head, bytes_accessed=8 * seq * head, transcendentals=pairs),
        compiler_params=pltpu.CompilerParams(vmem_limit_bytes=32 * 1024 * 1024, collective_id=cid, has_side_effects=True),
        name='attn_fwd',
    )(q, k, v)


RIGHT_0, RIGHT_1, RIGHT_F, LEFT_1, LEFT_0, LEFT_F, SIB, SIB_L0, SIB_L1, SIB_R0, SIB_R1, SIB_O0, SIB_O1 = range(13)


def table_block(pos_row, freq_row):
    size = pos_row.shape[1]
    eye = lax.broadcasted_iota(jnp.int32, (size, size), 0) == lax.broadcasted_iota(jnp.int32, (size, size), 1)
    pos = jnp.sum(jnp.where(eye, jnp.broadcast_to(pos_row, (size, size)), 0.0), axis=1, keepdims=True)
    angle = pos / ROPE_SCALE * freq_row
    turn = jnp.floor(angle * (2.0 / math.pi) + 0.5)
    rest = angle
    for part in HALF_PI:
        rest = rest - turn * part
    sq = rest * rest
    sin_r = rest + rest * sq * (-1.6666654611e-1 + sq * (8.3321608736e-3 + sq * -1.9515295891e-4))
    cos_r = 1.0 - 0.5 * sq + sq * sq * (4.166664568298827e-2 + sq * (-1.388731625493765e-3 + sq * 2.443315711809948e-5))
    quarter = turn - 4.0 * jnp.floor(turn * 0.25)
    odd = (quarter == 1.0) | (quarter == 3.0)
    cosines = jnp.where(odd, sin_r, cos_r)
    sines = jnp.where(odd, cos_r, sin_r)
    cosines = jnp.where((quarter == 1.0) | (quarter == 2.0), -cosines, cosines)
    sines = jnp.where(quarter >= 2.0, -sines, sines)
    return cosines, sines


def first_kernel(group, x_ref, pos_ref, freq_ref, wpre_ref, qn_ref, kn_ref, wq_ref, wk_ref, wv_ref,
                 full_ref, qr_ref, kr_ref, v_ref, qw_ref, kw_ref, cos_ref, sin_ref, o_ref, lse_ref, tok_ref,
                 buf, w_ref, pos_all, s_scr, acc, o_send, o_recv, send_sem, recv_sem, out_sem, w_sem, p_send, p_recv):
    batch, blk, _ = x_ref.shape
    head = qn_ref.shape[1]
    chips = group // 2
    me = lax.axis_index('sp')
    core, chip = lax.rem(me, 2), me // 2

    def device(chip_step, other):
        return 2 * lax.rem(chip + chips + chip_step, chips) + (1 - core if other else core)

    right, left, far, sib = device(1, False), device(-1, False), device(2, False), device(0, True)
    half = blk // 2
    halves = [pl.ds(0, half), pl.ds(half, half)]
    loads = [pltpu.make_async_copy(ref.at[:, block_of(index, head)], w_ref.at[:, pl.ds(place * head, head)], w_sem.at[place])
             for place, (ref, index) in enumerate(((wq_ref, me), (wk_ref, chip), (wv_ref, chip)))]
    for load in loads:
        load.start()

    @pl.loop(0, batch * 4)
    def _(t):
        rows = block_of(lax.rem(t, 4), blk // 4)
        x = x_ref[t // 4, rows, :].astype(F32)
        inv = lax.rsqrt(jnp.mean(x * x, axis=-1, keepdims=True) + EPS)
        buf[t // 4, me, rows, :] = (x * inv * (1.0 + wpre_ref[...])).astype(BF)

    others_barrier(group, me)

    def pos_copy(step):
        return pltpu.make_async_remote_copy(
            src_ref=pos_ref,
            dst_ref=pos_all.at[me],
            send_sem=p_send.at[step],
            recv_sem=p_recv.at[step],
            device_id={'sp': lax.rem(me + step, group)},
            device_id_type=MESH,
        )

    for step in range(1, group):
        pos_copy(step).start()

    def send(b, which, owner, rows, to):
        return pltpu.make_async_remote_copy(
            src_ref=buf.at[b, owner, rows],
            dst_ref=buf.at[b, owner, rows],
            send_sem=send_sem.at[b, which],
            recv_sem=recv_sem.at[b, which],
            device_id={'sp': to},
            device_id_type=MESH,
        )

    def plan(b):
        table = {}
        for which, rows, to in ((RIGHT_0, 0, right), (RIGHT_1, 1, right), (LEFT_1, 1, left), (LEFT_0, 0, left)):
            table[which] = send(b, which, me, halves[rows], to)
        table[SIB] = send(b, SIB, me, pl.ds(0, blk), sib)
        table[RIGHT_F] = send(b, RIGHT_F, left, halves[0], right)
        table[LEFT_F] = send(b, LEFT_F, right, halves[1], left)
        for which, owner, rows in ((SIB_L0, left, 0), (SIB_L1, left, 1), (SIB_R0, right, 0), (SIB_R1, right, 1), (SIB_O0, far, 0), (SIB_O1, far, 1)):
            table[which] = send(b, which, owner, halves[rows], sib)
        return table

    plans = [plan(b) for b in range(batch)]

    def go(b, *which):
        for w in which:
            plans[b][w].start()

    def got(b, *which):
        for w in which:
            plans[b][w].wait_recv()

    def out_copy(b, owner):
        return pltpu.make_async_copy(buf.at[b, owner], full_ref.at[b, block_of(owner, blk), :], out_sem.at[b, owner])

    def norm_rope_block(raw, weight, cosines, sines):
        x = raw.astype(F32)
        normed = x * lax.rsqrt(jnp.mean(x * x, axis=-1, keepdims=True) + EPS) * (1.0 + weight)
        first, second = normed[:, :head // 2], normed[:, head // 2:]
        return jnp.concatenate([first * cosines - second * sines, second * cosines + first * sines], axis=1).astype(BF)

    def project(b, owner):
        out_copy(b, owner).start()
        rows = block_of(owner, blk)
        qkv = nn(buf[b, owner], w_ref[...]).astype(BF)
        cosines, sines = cos_ref[rows, :], sin_ref[rows, :]
        q_raw, k_raw = qkv[:, :head], qkv[:, head:2 * head]
        qw_ref[b, rows, :] = q_raw
        kw_ref[b, rows, :] = k_raw
        v_ref[b, rows, :] = qkv[:, 2 * head:]
        qr_ref[b, rows, :] = norm_rope_block(q_raw, qn_ref[...], cosines, sines)
        kr_ref[b, rows, :] = norm_rope_block(k_raw, kn_ref[...], cosines, sines)

    def project_own(b):
        got(b, SIB)

        @pl.loop(0, 2)
        def _(t):
            project(b, 2 * chip + lax.rem(core + t, 2))

    def project_near(b):
        got(b, SIB_L0, SIB_R1, SIB_L1, SIB_R0)

        @pl.loop(0, 4)
        def _(t):
            project(b, 2 * lax.rem(chip + 1 + 2 * lax.rem(t, 2), chips) + lax.rem(core + t // 2, 2))

    def project_far(b):
        got(b, RIGHT_F, LEFT_F)
        go(b, SIB_O0, SIB_O1)
        got(b, SIB_O0, SIB_O1)

        @pl.loop(0, 2)
        def _(t):
            project(b, 2 * lax.rem(chip + 2, chips) + lax.rem(core + t, 2))

    go(0, RIGHT_0, LEFT_1, RIGHT_1, LEFT_0, SIB)
    pos_all[me] = pos_ref[...]
    for step in range(1, group):
        pos_copy(step).wait()

    @pl.loop(0, group)
    def _(owner):
        cosines, sines = table_block(pos_all[owner], freq_ref[...])
        cos_ref[block_of(owner, blk), :] = cosines
        sin_ref[block_of(owner, blk), :] = sines

    for load in loads:
        load.wait()
    project_own(0)
    for b in range(batch):
        if b:
            project_own(b)
            attention = Attention(group, me, qr_ref.at[b - 1], kr_ref.at[b - 1], v_ref.at[b - 1], o_ref, lse_ref, tok_ref, s_scr, acc, o_send, o_recv)
            attention.blocks(0, group // 2)
        got(b, RIGHT_0, LEFT_1)
        go(b, RIGHT_F, LEFT_F, SIB_L0, SIB_R1)
        if b + 1 < batch:
            go(b + 1, RIGHT_0, LEFT_1, RIGHT_1, LEFT_0, SIB)
        if b:
            attention.blocks(group // 2, group)
            attention.flush()
        got(b, RIGHT_1, LEFT_0)
        go(b, SIB_L1, SIB_R0)
        project_near(b)
        project_far(b)
    attention.finish()
    for b in range(batch):
        for w in range(13):
            plans[b][w].wait_send()

        @pl.loop(0, group)
        def _(owner):
            out_copy(b, owner).wait()


def first(x, pos, freq, w_pre, q_norm, k_norm, w_q, w_k, w_v, group, cid):
    batch, blk, width = x.shape
    head = q_norm.shape[0]
    seq = group * blk
    assert batch == 2 and group == 8
    heads_out = jax.ShapeDtypeStruct((batch, seq, head), BF)
    table = jax.ShapeDtypeStruct((seq, head // 2), F32)
    vmem = pl.BlockSpec(memory_space=pltpu.VMEM)
    anywhere = pl.BlockSpec(memory_space=pl.ANY)
    dma = pltpu.SemaphoreType.DMA
    return pl.pallas_call(
        functools.partial(first_kernel, group),
        out_shape=(jax.ShapeDtypeStruct((batch, seq, width), BF),) + (heads_out,) * 5 + (table,) * 2 + attn_outs(group, blk, seq, head),
        in_specs=[vmem] * 6 + [anywhere] * 3,
        out_specs=(anywhere,) + (vmem,) * 10,
        scratch_shapes=[pltpu.VMEM((batch, group, blk, width), BF), pltpu.VMEM((width, 3 * head), BF), pltpu.VMEM((group, 1, blk), F32)]
        + attn_scratch(group, blk, seq, head)
        + [dma((batch, 13)), dma((batch, 13)), dma((batch, group)), dma((3,)), dma((group,)), dma((group,))],
        cost_estimate=pl.CostEstimate(flops=90 * 10 ** 9, bytes_accessed=2 * batch * seq * width, transcendentals=seq * seq),
        compiler_params=pltpu.CompilerParams(vmem_limit_bytes=60 * 1024 * 1024, collective_id=cid, has_side_effects=True),
        name='first',
    )(x, pos, freq, w_pre[None, :], q_norm[None, :], k_norm[None, :], w_q, w_k, w_v)


def bwd_kernel(q_ref, k_ref, v_ref, do_ref, lse_ref, dl_ref, dq_ref, dk_ref, dv_ref, dq_acc):
    seq, head = q_ref.shape
    scale = head ** -0.5
    upper = lax.broadcasted_iota(jnp.int32, (BWD_BLK, BWD_BLK), 0) <= lax.broadcasted_iota(jnp.int32, (BWD_BLK, BWD_BLK), 1)
    dq_acc[...] = jnp.zeros_like(dq_acc)
    dk_ref[...] = jnp.zeros_like(dk_ref)
    dv_ref[...] = jnp.zeros_like(dv_ref)

    @pl.loop(0, seq // BWD_BLK)
    def _(j):
        cols = pl.ds(pl.multiple_of(j * BWD_BLK, BWD_BLK), BWD_BLK)
        k = k_ref[cols, :]
        v = v_ref[cols, :]

        def step(i, masked):
            rows = pl.ds(pl.multiple_of(i * BWD_BLK, BWD_BLK), BWD_BLK)
            q = q_ref[rows, :]
            do = do_ref[rows, :]
            st = nt(k, q) * scale
            if masked:
                st = jnp.where(upper, st, NEG_BIG)
            pt = jnp.exp(st - lse_ref[0:1, rows])
            dpt = nt(v, do)
            dst = (pt * (dpt - dl_ref[0:1, rows]) * scale).astype(BF)
            dv_ref[cols, :] += nn(pt.astype(BF), do)
            dk_ref[cols, :] += nn(dst, q)
            dq_acc[rows, :] += tn(dst, k)

        step(j, True)

        @pl.loop(j + 1, seq // BWD_BLK)
        def _(i):
            step(i, False)

    dq_ref[...] = dq_acc[...].astype(BF)


def attn_bwd(q, k, v, do, lse, delta):
    seq, head = q.shape
    blk = BWD_BLK
    pairs = seq * (seq + blk) // 2
    return pl.pallas_call(
        bwd_kernel,
        out_shape=(jax.ShapeDtypeStruct((seq, head), BF), jax.ShapeDtypeStruct((seq, head), F32), jax.ShapeDtypeStruct((seq, head), F32)),
        in_specs=[pl.BlockSpec(memory_space=pltpu.VMEM)] * 6,
        out_specs=(pl.BlockSpec(memory_space=pltpu.VMEM),) * 3,
        scratch_shapes=[pltpu.VMEM((seq, head), F32)],
        cost_estimate=pl.CostEstimate(flops=10 * pairs * head, bytes_accessed=20 * seq * head, transcendentals=pairs),
        compiler_params=pltpu.CompilerParams(vmem_limit_bytes=32 * 1024 * 1024),
        name='attn_bwd',
    )(q, k, v, do, lse, delta)


def move_kernel(*refs):
    for src, dst in zip(refs[:len(refs) // 2], refs[len(refs) // 2:]):
        dst[...] = src[...].reshape(dst.shape)


def move(grid, out_shapes, in_specs, out_specs, operands):
    size = sum(s.size for s in out_shapes)
    return pl.pallas_call(
        move_kernel,
        grid=grid,
        out_shape=out_shapes,
        in_specs=in_specs,
        out_specs=out_specs,
        cost_estimate=pl.CostEstimate(flops=20 * size, bytes_accessed=4 * size, transcendentals=0),
        compiler_params=pltpu.CompilerParams(vmem_limit_bytes=32 * 1024 * 1024),
    )(*operands)


def spread_q(parts):
    group, rows, head = parts.shape
    return move((group,), (jax.ShapeDtypeStruct((rows, group * head), BF),),
                [pl.BlockSpec((1, rows, head), lambda c: (c, 0, 0))], (pl.BlockSpec((rows, head), lambda c: (0, c)),), (parts,))[0]


def spread_kv(parts):
    group, rows, head = parts.shape
    shape = jax.ShapeDtypeStruct((rows, group // 2 * head), BF)
    out = pl.BlockSpec((rows, head), lambda c: (0, c))
    return move((group // 2,), (shape, shape),
                [pl.BlockSpec((1, rows, head), lambda c: (2 * c, 0, 0)), pl.BlockSpec((1, rows, head), lambda c: (2 * c + 1, 0, 0))], (out, out), (parts, parts))


def place(whole):
    rows, wide = whole.shape
    spec = pl.BlockSpec((rows // 8, wide), lambda r: (r, 0))
    return move((8,), (jax.ShapeDtypeStruct((rows, wide), BF),), [spec], (spec,), (whole,))[0]


def solution(mesh):
    group = mesh.shape['sp']

    def device_step(x_in, dy_in, positions, w_q, w_k, w_v, w_o, w_pre, w_post, q_norm, k_norm):
        batch, seq_loc, width = x_in.shape
        head = q_norm.shape[0]
        heads = w_q.shape[1] // head
        kv_heads = w_k.shape[1] // head
        rep = group // kv_heads
        assert heads == group and rep == 2
        me = lax.axis_index('sp')
        even = (me % rep) == 0
        swap = [(d, d ^ 1) for d in range(group)]
        wo_mine = lax.dynamic_slice(w_o, (me * head, 0), (head, width))

        x_f32 = [x_in[b].astype(F32) for b in range(batch)]
        dy_f32 = [dy_in[b].astype(F32) for b in range(batch)]
        inv_freq = ROPE_BASE ** (-jnp.arange(head // 2, dtype=F32) * 2.0 / head)
        (a_both, q_both, k_both, v_both, q_raw, k_raw, cosines, sines, o_first, lse_first, tok_first) = first(
            x_in, positions.astype(F32)[None, :], inv_freq[None, :], w_pre, q_norm, k_norm, w_q, w_k, w_v, group, 0)
        roper = functools.partial(norm_rope, cosines=cosines, sines=sines)
        a_all = [a_both[b] for b in range(batch)]

        saved = []
        dproj_all = []
        y_out, dw_post = [], 0.0
        for b in range(batch):
            q_rot, k_rot, v_raw = q_both[b], k_both[b], v_both[b]
            _, q_pull = jax.vjp(roper, q_raw[b], q_norm)
            _, k_pull = jax.vjp(roper, k_raw[b], k_norm)
            if b == 0:
                o, lse, o_tok = o_first, lse_first, tok_first
            else:
                o, lse, o_tok = attn_fwd(q_rot, k_rot, v_raw, group, b)
            saved.append((q_rot, k_rot, v_raw, o, lse, q_pull, k_pull))
            proj = nn(o_tok, w_o).astype(BF)
            post, post_pull = jax.vjp(post_norm, proj, w_post)
            y_out.append((x_f32[b] + post).astype(BF))
            d_proj, dwp = post_pull(dy_f32[b])
            dw_post = dw_post + dwp
            dproj_all.append(lax.all_gather(d_proj, 'sp', axis=0, tiled=True))
            if b + 1 < batch:
                q_both, _ = lax.optimization_barrier((q_both, d_proj))

        dproj_all[0], _ = lax.optimization_barrier((dproj_all[0], d_proj))
        d_mine, dqkv_tok = [], []
        dq_norm = dk_norm = 0.0
        dw_o = 0.0
        for b in range(batch):
            q_rot, k_rot, v_raw, o, lse, q_pull, k_pull = saved[b]
            if b:
                dproj_all[b], _ = lax.optimization_barrier((dproj_all[b], d_mine[b - 1]))
            dw_o = dw_o + tn(o, dproj_all[b])
            if b + 1 == batch:
                dw_o_all = lax.all_gather(dw_o.astype(BF), 'sp', axis=0, tiled=True)
            d_o = nt(dproj_all[b], wo_mine).astype(BF)
            delta = jnp.sum(d_o.astype(F32) * o.astype(F32), axis=1)[None, :]
            dq_rot, dk_part, dv_part = attn_bwd(q_rot, k_rot, v_raw, d_o, lse.reshape(1, -1), delta)
            other = lax.ppermute(jnp.where(even, dv_part, dk_part), 'sp', swap)
            dkv = (jnp.where(even, dk_part, dv_part) + other).astype(BF)
            dq_proj, dqn = q_pull(dq_rot)
            dk_proj, dkn = k_pull(dkv)
            dq_norm = dq_norm + dqn
            dk_norm = dk_norm + jnp.where(even, dkn, 0.0)
            d_two = jnp.concatenate([dq_proj, jnp.where(even, dk_proj, dkv)], axis=1)
            d_mine.append(d_two)
            if b:
                d_two, dqkv_tok[b - 1] = lax.optimization_barrier((d_two, dqkv_tok[b - 1]))
            dqkv_tok.append(lax.all_to_all(d_two, 'sp', 0, 1, tiled=True))

        dw_q_part = sum(tn(a_all[b], d_mine[b][:, :head]) for b in range(batch)).astype(BF)
        dw_q_parts = lax.all_gather(dw_q_part, 'sp', axis=0, tiled=False)
        dw_kv_part = sum(tn(a_all[b], d_mine[b][:, head:]) for b in range(batch)).astype(BF)
        dw_kv_parts = lax.all_gather(dw_kv_part, 'sp', axis=0, tiled=False)
        dw_o_all = place(dw_o_all)
        dqkv_tok[1], dw_o_all = lax.optimization_barrier((dqkv_tok[1], dw_o_all))

        d_tok = jnp.concatenate(dqkv_tok, axis=0)
        d_tok = [d_tok[:, j * head:(j + 1) * head] for j in range(2 * group)]
        d_normed = (nt(jnp.concatenate(d_tok[0::2], axis=1), w_q)
                    + nt(jnp.concatenate(d_tok[1::4], axis=1), w_k)
                    + nt(jnp.concatenate(d_tok[3::4], axis=1), w_v)).astype(BF).reshape(batch, seq_loc, width)
        _, pre_pull = jax.vjp(pre_norm, x_in.astype(F32), w_pre)
        dx_norm, dw_pre = pre_pull(d_normed)
        dx_out = (dy_in.astype(F32) + dx_norm).astype(BF)
        dw_q_all = spread_q(dw_q_parts)
        dw_k_all, dw_v_all = spread_kv(dw_kv_parts)
        small = lax.psum((dw_pre, dw_post, dq_norm, dk_norm), 'sp')
        return (jnp.stack(y_out), dx_out, dw_q_all, dw_k_all, dw_v_all, dw_o_all) + small

    token_spec = P('dp', 'sp', None)
    return jax.shard_map(device_step, mesh=mesh,
                         in_specs=(token_spec, token_spec, P(('dp', 'sp')), P(None, None), P(None, None), P(None, None), P(None, None), P(None), P(None), P(None), P(None)),
                         out_specs=(token_spec, token_spec, P('dp', None), P('dp', None), P('dp', None), P('dp', None), P('dp'), P('dp'), P('dp'), P('dp')),
                         check_vma=False)
```

```python
import functools
import math
import jax
import jax.numpy as jnp
from jax import lax
from jax.experimental import pallas as pl
from jax.experimental.pallas import tpu as pltpu
from jax.sharding import PartitionSpec as P

EPS = 1e-6
ROPE_BASE = 1000000.0
ROPE_SCALE = 8.0
NEG_BIG = -1e30
HALF_PI = (1.5625, 0.0081787109375, 0.00011730194091796875, 3.129243850708008e-07, 9.920935796805404e-10)
BWD_BLK = 256
BF = jnp.bfloat16
F32 = jnp.float32
MESH = pl.DeviceIdType.MESH


def rms_scale(x_f32, weight):
    inv_rms = lax.rsqrt(jnp.mean(x_f32 * x_f32, axis=-1, keepdims=True) + EPS)
    return x_f32 * inv_rms * (1.0 + weight)


def pre_norm(x_f32, weight):
    return rms_scale(x_f32, weight).astype(BF)


def norm_rope(head_bf, weight, cosines, sines):
    half_dim = head_bf.shape[-1] // 2
    normed = rms_scale(head_bf.astype(F32), weight)
    first = normed[..., :half_dim]
    second = normed[..., half_dim:]
    rotated = jnp.concatenate([first * cosines - second * sines, second * cosines + first * sines], axis=-1)
    return rotated.astype(BF)


def nt(lhs, rhs):
    return lax.dot_general(lhs, rhs, (((1,), (1,)), ((), ())), preferred_element_type=F32)


def nn(lhs, rhs):
    return lax.dot_general(lhs, rhs, (((1,), (0,)), ((), ())), preferred_element_type=F32)


def tn(lhs, rhs):
    return lax.dot_general(lhs, rhs, (((0,), (0,)), ((), ())), preferred_element_type=F32)


def others_barrier(group, me):
    barrier = pltpu.get_barrier_semaphore()
    for step in range(1, group):
        pl.semaphore_signal(barrier, inc=1, device_id={'sp': lax.rem(me + step, group)}, device_id_type=MESH)
    pl.semaphore_wait(barrier, group - 1)


def block_of(index, size):
    return pl.ds(pl.multiple_of(index * size, size), size)


def fold(x, op):
    out = x[:, :128]
    for c in range(1, x.shape[1] // 128):
        out = op(out, x[:, c * 128:(c + 1) * 128])
    return out


def diagonal(size):
    return lax.broadcasted_iota(jnp.int32, (size, size), 0) == lax.broadcasted_iota(jnp.int32, (size, size), 1)


def as_row(column):
    size = column.shape[0]
    return jnp.sum(jnp.where(diagonal(size), jnp.broadcast_to(column, (size, size)), 0.0), axis=0, keepdims=True)


def as_column(row):
    size = row.shape[1]
    return jnp.sum(jnp.where(diagonal(size), jnp.broadcast_to(row, (size, size)), 0.0), axis=1, keepdims=True)


class Attention:
    def __init__(self, group, me, b, q_ref, k_ref, v_ref, o_ref, lse_ref, tok_ref, s_scr, acc, send_sem, recv_sem):
        self.group, self.me, self.b = group, me, b
        self.refs = q_ref, k_ref, v_ref, o_ref, lse_ref, tok_ref, s_scr, acc
        self.sems = send_sem, recv_sem
        self.blk, self.head = acc.shape
        self.mine = block_of(me, self.head)

    def copy_to(self, step):
        o_ref, tok_ref = self.refs[3], self.refs[5]
        peer = lax.rem(self.me + step, self.group)
        return pltpu.make_async_remote_copy(
            src_ref=o_ref.at[block_of(peer, self.blk), :],
            dst_ref=tok_ref.at[pl.ds(self.b * self.blk, self.blk), self.mine],
            send_sem=self.sems[0].at[self.b, step],
            recv_sem=self.sems[1].at[self.b, step],
            device_id={'sp': peer},
            device_id_type=MESH,
        )

    def blocks(self, first, last):
        q_ref, k_ref, v_ref, o_ref, lse_ref, _, s_scr, acc = self.refs
        blk, head = self.blk, self.head
        scale = head ** -0.5
        wide = 2 * blk
        ahead = lax.broadcasted_iota(jnp.int32, (blk, wide), 0) - lax.broadcasted_iota(jnp.int32, (blk, wide), 1)

        @pl.loop(first, last)
        def _(step):
            i = lax.rem(self.me + step, self.group)
            rows = block_of(i, blk)
            q = q_ref[rows, :]
            edge = i // 2
            cols = block_of(edge, wide)
            s = jnp.where(ahead + lax.rem(i, 2) * blk >= 0, nt(q, k_ref[cols, :]) * scale, NEG_BIG)
            s_scr[:, cols] = s

            def pass1(j, m):
                cols = block_of(j, wide)
                s = nt(q, k_ref[cols, :]) * scale
                s_scr[:, cols] = s
                return jnp.maximum(m, fold(s, jnp.maximum))

            m = lax.fori_loop(0, edge, pass1, fold(s, jnp.maximum))
            m = jnp.max(m, axis=1, keepdims=True)

            @pl.when(step > 1)
            def _():
                self.copy_to(step - 1).start()

            def pass2(j, l):
                cols = block_of(j, wide)
                p = jnp.exp(s_scr[:, cols] - m)
                s_scr[:, cols] = p
                return l + fold(p, jnp.add)

            l = lax.fori_loop(0, edge + 1, pass2, jnp.zeros((blk, min(128, blk)), F32))
            l = jnp.sum(l, axis=1, keepdims=True)
            inv = 1.0 / l
            acc[...] = jnp.zeros_like(acc)

            @pl.loop(0, edge + 1)
            def _(j):
                cols = block_of(j, wide)
                acc[...] += nn((s_scr[:, cols] * inv).astype(BF), v_ref[cols, :])

            o_ref[rows, :] = acc[...].astype(BF)
            lse_ref[:, rows] = as_row(m + jnp.log(l))

    def flush(self):
        o_ref, tok_ref = self.refs[3], self.refs[5]
        tok_ref[pl.ds(self.b * self.blk, self.blk), self.mine] = o_ref[block_of(self.me, self.blk), :]
        self.copy_to(self.group - 1).start()

    def finish(self):
        @pl.loop(1, self.group)
        def _(step):
            self.copy_to(step).wait()


RIGHT_0, RIGHT_1, RIGHT_F, LEFT_1, LEFT_0, LEFT_F, SIB, SIB_L0, SIB_L1, SIB_R0, SIB_R1, SIB_O0, SIB_O1 = range(13)


class Ring:
    def __init__(self, group, me, buf, send_sem, recv_sem):
        self.me, self.chips = me, group // 2
        self.core, self.chip = lax.rem(me, 2), me // 2
        self.buf, self.sems = buf, (send_sem, recv_sem)
        self.blk = buf.shape[2]
        self.right, self.left, self.far = self.device(1, 0), self.device(-1, 0), self.device(2, 0)
        self.plans = [self.plan(b) for b in range(buf.shape[0])]

    def device(self, chip_step, other):
        return 2 * lax.rem(self.chip + self.chips + chip_step, self.chips) + lax.rem(self.core + other, 2)

    def send(self, b, which, owner, rows, to):
        place = self.buf.at[b, owner, rows]
        return pltpu.make_async_remote_copy(
            src_ref=place,
            dst_ref=place,
            send_sem=self.sems[0].at[b, which],
            recv_sem=self.sems[1].at[b, which],
            device_id={'sp': to},
            device_id_type=MESH,
        )

    def plan(self, b):
        me, right, left, far, sib = self.me, self.right, self.left, self.far, self.device(0, 1)
        half = self.blk // 2
        halves = [pl.ds(0, half), pl.ds(half, half)]
        routes = ((RIGHT_0, me, 0, right), (RIGHT_1, me, 1, right), (LEFT_1, me, 1, left), (LEFT_0, me, 0, left),
                  (RIGHT_F, left, 0, right), (LEFT_F, right, 1, left), (SIB_L0, left, 0, sib), (SIB_L1, left, 1, sib),
                  (SIB_R0, right, 0, sib), (SIB_R1, right, 1, sib), (SIB_O0, far, 0, sib), (SIB_O1, far, 1, sib))
        table = {which: self.send(b, which, owner, halves[rows], to) for which, owner, rows, to in routes}
        table[SIB] = self.send(b, SIB, me, pl.ds(0, self.blk), sib)
        return table

    def go(self, b, *which):
        for w in which:
            self.plans[b][w].start()

    def got(self, b, *which):
        for w in which:
            self.plans[b][w].wait_recv()

    def open(self, b):
        self.go(b, RIGHT_0, LEFT_1, RIGHT_1, LEFT_0, SIB)

    def turn(self, b):
        self.got(b, RIGHT_0, LEFT_1)
        self.go(b, RIGHT_F, LEFT_F, SIB_L0, SIB_R1)

    def near(self, b):
        self.got(b, RIGHT_1, LEFT_0)
        self.go(b, SIB_L1, SIB_R0)

    def each_own(self, b, work):
        self.got(b, SIB)

        @pl.loop(0, 2)
        def _(t):
            work(b, self.device(0, t))

    def each_near(self, b, work):
        self.got(b, SIB_L0, SIB_R1, SIB_L1, SIB_R0)

        @pl.loop(0, 4)
        def _(t):
            work(b, self.device(1 + 2 * lax.rem(t, 2), t // 2))

    def each_far(self, b, work):
        self.got(b, RIGHT_F, LEFT_F)
        self.go(b, SIB_O0, SIB_O1)
        self.got(b, SIB_O0, SIB_O1)

        @pl.loop(0, 2)
        def _(t):
            work(b, self.device(2, t))

    def sent(self):
        for plan in self.plans:
            for copy in plan.values():
                copy.wait_send()


def table_block(pos_row, freq_row):
    angle = as_column(pos_row) / ROPE_SCALE * freq_row
    turn = jnp.floor(angle * (2.0 / math.pi) + 0.5)
    rest = angle
    for part in HALF_PI:
        rest = rest - turn * part
    sq = rest * rest
    sin_r = rest + rest * sq * (-1.6666654611e-1 + sq * (8.3321608736e-3 + sq * -1.9515295891e-4))
    cos_r = 1.0 - 0.5 * sq + sq * sq * (4.166664568298827e-2 + sq * (-1.388731625493765e-3 + sq * 2.443315711809948e-5))
    quarter = turn - 4.0 * jnp.floor(turn * 0.25)
    odd = (quarter == 1.0) | (quarter == 3.0)
    cosines = jnp.where(odd, sin_r, cos_r)
    sines = jnp.where(odd, cos_r, sin_r)
    cosines = jnp.where((quarter == 1.0) | (quarter == 2.0), -cosines, cosines)
    sines = jnp.where(quarter >= 2.0, -sines, sines)
    return cosines, sines


def first_kernel(group, batch, x_ref, pos_ref, freq_ref, wpre_ref, qn_ref, kn_ref, wq_ref, wk_ref, wv_ref, full_ref, cos_out, sin_out, tok_ref, *rest):
    per_out = [rest[b * 7:(b + 1) * 7] for b in range(batch)]
    buf, w_ref, pos_all, s_scr, acc, cos_ref, sin_ref, o_send, o_recv, send_sem, recv_sem, out_sem, w_sem, p_send, p_recv, keep_sem, table_sem = rest[batch * 7:batch * 7 + 17]
    kept = rest[batch * 7 + 17:]
    per = [kept[b * 6:(b + 1) * 6] + (per_out[b][6],) for b in range(batch)]
    outward = [[pltpu.make_async_copy(per[b][n], per_out[b][n], keep_sem.at[b, n]) for n in range(6)] for b in range(batch)]
    tables = [pltpu.make_async_copy(cos_ref, cos_out, table_sem.at[0]), pltpu.make_async_copy(sin_ref, sin_out, table_sem.at[1])]
    blk, _ = x_ref.shape[1:]
    head = qn_ref.shape[1]
    me = lax.axis_index('sp')
    loads = [pltpu.make_async_copy(ref.at[:, block_of(index, head)], w_ref.at[:, pl.ds(place * head, head)], w_sem.at[place])
             for place, (ref, index) in enumerate(((wq_ref, me), (wk_ref, me // 2), (wv_ref, me // 2)))]
    for load in loads:
        load.start()

    @pl.loop(0, batch * 4)
    def _(t):
        rows = block_of(lax.rem(t, 4), blk // 4)
        x = x_ref[t // 4, rows, :].astype(F32)
        inv = lax.rsqrt(jnp.mean(x * x, axis=-1, keepdims=True) + EPS)
        buf[t // 4, me, rows, :] = (x * inv * (1.0 + wpre_ref[...])).astype(BF)

    others_barrier(group, me)
    ring = Ring(group, me, buf, send_sem, recv_sem)

    def pos_copy(step):
        return pltpu.make_async_remote_copy(
            src_ref=pos_ref,
            dst_ref=pos_all.at[me],
            send_sem=p_send.at[step],
            recv_sem=p_recv.at[step],
            device_id={'sp': lax.rem(me + step, group)},
            device_id_type=MESH,
        )

    for step in range(1, group):
        pos_copy(step).start()

    def out_copy(b, owner):
        return pltpu.make_async_copy(buf.at[b, owner], full_ref.at[b, block_of(owner, blk), :], out_sem.at[b, owner])

    def norm_rope_block(raw, weight, cosines, sines):
        x = raw.astype(F32)
        normed = x * lax.rsqrt(jnp.mean(x * x, axis=-1, keepdims=True) + EPS) * (1.0 + weight)
        first, second = normed[:, :head // 2], normed[:, head // 2:]
        return jnp.concatenate([first * cosines - second * sines, second * cosines + first * sines], axis=1).astype(BF)

    def project(b, owner):
        q_ref, k_ref, v_ref, qw_ref, kw_ref = per[b][:5]
        out_copy(b, owner).start()
        rows = block_of(owner, blk)
        qkv = nn(buf[b, owner], w_ref[...]).astype(BF)
        cosines, sines = cos_ref[rows, :], sin_ref[rows, :]
        q_raw, k_raw = qkv[:, :head], qkv[:, head:2 * head]
        qw_ref[rows, :] = q_raw
        kw_ref[rows, :] = k_raw
        v_ref[rows, :] = qkv[:, 2 * head:]
        q_ref[rows, :] = norm_rope_block(q_raw, qn_ref[...], cosines, sines)
        k_ref[rows, :] = norm_rope_block(k_raw, kn_ref[...], cosines, sines)

    ring.open(0)
    pos_all[me] = pos_ref[...]
    for step in range(1, group):
        pos_copy(step).wait()

    @pl.loop(0, group)
    def _(owner):
        cosines, sines = table_block(pos_all[owner], freq_ref[...])
        cos_ref[block_of(owner, blk), :] = cosines
        sin_ref[block_of(owner, blk), :] = sines

    for copy in tables:
        copy.start()
    for load in loads:
        load.wait()
    attention = [Attention(group, me, b, *per[b][:3], *per[b][5:], tok_ref, s_scr, acc, o_send, o_recv) for b in range(batch)]
    ring.each_own(0, project)
    for b in range(batch):
        if b:
            ring.each_own(b, project)
            attention[b - 1].blocks(0, group // 2)
        ring.turn(b)
        if b + 1 < batch:
            ring.open(b + 1)
        if b:
            attention[b - 1].blocks(group // 2, group)
            attention[b - 1].flush()
            outward[b - 1][5].start()
        ring.near(b)
        ring.each_near(b, project)
        ring.each_far(b, project)
        for copy in outward[b][:5]:
            copy.start()
    attention[-1].blocks(0, group)
    attention[-1].flush()
    outward[-1][5].start()
    for b in range(batch):
        attention[b].finish()
    ring.sent()
    for copy in tables + sum(outward, []):
        copy.wait()
    for b in range(batch):
        @pl.loop(0, group)
        def _(owner):
            out_copy(b, owner).wait()


VMEM = pl.BlockSpec(memory_space=pltpu.VMEM)
ANYWHERE = pl.BlockSpec(memory_space=pl.ANY)
DMA = pltpu.SemaphoreType.DMA


def first(x, pos, freq, w_pre, q_norm, k_norm, w_q, w_k, w_v, group, cid):
    batch, blk, width = x.shape
    head = q_norm.shape[0]
    seq = group * blk
    assert group == 8
    heads_out = jax.ShapeDtypeStruct((seq, head), BF)
    table = jax.ShapeDtypeStruct((seq, head // 2), F32)
    outs = pl.pallas_call(
        functools.partial(first_kernel, group, batch),
        out_shape=(jax.ShapeDtypeStruct((batch, seq, width), BF), table, table, jax.ShapeDtypeStruct((batch * blk, group * head), BF))
        + ((heads_out,) * 6 + (jax.ShapeDtypeStruct((1, seq), F32),)) * batch,
        in_specs=[VMEM] * 6 + [ANYWHERE] * 3,
        out_specs=(ANYWHERE,) * 3 + (VMEM,) + ((ANYWHERE,) * 6 + (VMEM,)) * batch,
        scratch_shapes=[pltpu.VMEM((batch, group, blk, width), BF), pltpu.VMEM((width, 3 * head), BF), pltpu.VMEM((group, 1, blk), F32),
                        pltpu.VMEM((blk, seq), F32), pltpu.VMEM((blk, head), F32), pltpu.VMEM((seq, head // 2), F32), pltpu.VMEM((seq, head // 2), F32),
                        DMA((batch, group)), DMA((batch, group)), DMA((batch, 13)), DMA((batch, 13)), DMA((batch, group)), DMA((3,)), DMA((group,)), DMA((group,)),
                        DMA((batch, 6)), DMA((2,))] + [pltpu.VMEM((seq, head), BF)] * (6 * batch),
        cost_estimate=pl.CostEstimate(flops=90 * 10 ** 9, bytes_accessed=2 * batch * seq * width, transcendentals=seq * seq),
        compiler_params=pltpu.CompilerParams(vmem_limit_bytes=62 * 1024 * 1024, collective_id=cid, has_side_effects=True),
        name='first',
    )(x, pos, freq, w_pre[None, :], q_norm[None, :], k_norm[None, :], w_q, w_k, w_v)
    return outs[:4] + (tuple(outs[4 + 7 * b:11 + 7 * b] for b in range(batch)),)


def second_kernel(group, batch, tok_ref, wpost_ref, lse_ref, wo_hbm, x_hbm, dy_hbm, *rest):
    late_hbm, rest = rest[:3 + batch], rest[3 + batch:]
    y_hbm, dwpost_ref, dwo_ref, dq_ref, dk_ref, dv_ref = rest[:6]
    do_refs, dl_refs, rest = rest[6:6 + batch], rest[6 + batch:6 + 2 * batch], rest[6 + 2 * batch:]
    buf, dq_acc, dwo_acc, wo_ref, x_ref, dy_ref, p_scr, send_sem, recv_sem, wo_sem, act_sem, late_sem, y_sem = rest[:13]
    late = rest[13:]
    q_ref, k_ref, v_ref = late[:3]
    o_refs = late[3:]
    blk, width = x_ref.shape[1:]
    head = dwo_ref.shape[0]
    me = lax.axis_index('sp')
    mine = block_of(me, head)
    part = width // wo_sem.shape[0]
    wo_loads = [pltpu.make_async_copy(wo_hbm.at[:, pl.ds(n * part, part)], wo_ref.at[:, pl.ds(n * part, part)], wo_sem.at[n]) for n in range(width // part)]
    act_loads = [[pltpu.make_async_copy(src.at[b], dst.at[b], act_sem.at[b, n]) for n, (src, dst) in enumerate(((x_hbm, x_ref), (dy_hbm, dy_ref)))] for b in range(batch)]
    late_loads = [pltpu.make_async_copy(src, dst, late_sem.at[n]) for n, (src, dst) in enumerate(zip(late_hbm, late))]
    for load in wo_loads + sum(act_loads, []) + late_loads:
        load.start()
    dwpost_ref[...] = jnp.zeros_like(dwpost_ref)
    dwo_acc[...] = jnp.zeros_like(dwo_acc)
    y_copies = [pltpu.make_async_copy(x_ref.at[b], y_hbm.at[b], y_sem.at[b]) for b in range(batch)]

    def project(b):
        for n in range(width // part):
            if b == 0:
                wo_loads[n].wait()
            p_scr[:, n * part:(n + 1) * part] = nn(tok_ref[b * blk:(b + 1) * blk, :], wo_ref[:, n * part:(n + 1) * part]).astype(BF)
        for load in act_loads[b]:
            load.wait()
        gain = 1.0 + wpost_ref[...]
        rows_each = 32

        @pl.loop(0, blk // rows_each)
        def _(t):
            rows = block_of(t, rows_each)
            p = p_scr[rows, :].astype(F32)
            dy = dy_ref[b, rows, :].astype(F32)
            inv = lax.rsqrt(jnp.mean(p * p, axis=-1, keepdims=True) + EPS)
            unit = p * inv
            x_ref[b, rows, :] = (x_ref[b, rows, :].astype(F32) + unit * gain).astype(BF)
            scaled = dy * gain
            dwpost_ref[...] += jnp.sum(dy * unit, axis=0, keepdims=True)
            buf[b, me, rows, :] = (inv * (scaled - unit * jnp.mean(scaled * unit, axis=-1, keepdims=True))).astype(BF)

        y_copies[b].start()

    project(0)
    others_barrier(group, me)
    ring = Ring(group, me, buf, send_sem, recv_sem)

    def work(b, owner):
        rows = block_of(owner, blk)
        chunk = buf[b, owner]
        o = o_refs[b][rows, :]
        d_o = nt(chunk, wo_ref[mine, :]).astype(BF)
        do_refs[b][rows, :] = d_o
        dl_refs[b][:, rows] = as_row(jnp.sum(d_o.astype(F32) * o.astype(F32), axis=1, keepdims=True))
        dwo_acc[...] += tn(o, chunk)

    def backward(first, last):
        bwd_blocks(first, last, q_ref, k_ref, v_ref, do_refs[0], lse_ref, dl_refs[0], dq_acc, dk_ref, dv_ref)

    ring.open(0)
    for b in range(1, batch):
        project(b)
    for load in late_loads:
        load.wait()
    ring.each_own(0, work)
    for b in range(batch):
        if b:
            ring.each_own(b, work)
            bwd_start(dq_acc, dk_ref, dv_ref)
            backward(0, 3)
        ring.turn(b)
        if b + 1 < batch:
            ring.open(b + 1)
        if b:
            backward(3, group)
            dq_ref[...] = dq_acc[...].astype(BF)
        ring.near(b)
        ring.each_near(b, work)
        ring.each_far(b, work)
    dwo_ref[...] = dwo_acc[...].astype(BF)
    ring.sent()
    for copy in y_copies:
        copy.wait()


def second(tok, w_o, x, dy, w_post, q, k, v, lse, outs, group, cid):
    batch, blk, width = x.shape
    seq, head = q.shape
    assert batch == 2 and group == 8
    wide = jax.ShapeDtypeStruct((seq, head), F32)
    half = jax.ShapeDtypeStruct((seq, head), BF)
    row = jax.ShapeDtypeStruct((1, seq), F32)
    res = pl.pallas_call(
        functools.partial(second_kernel, group, batch),
        out_shape=(jax.ShapeDtypeStruct(x.shape, BF), jax.ShapeDtypeStruct((1, width), F32), jax.ShapeDtypeStruct((head, width), BF), half, wide, wide)
        + (half,) * batch + (row,) * batch,
        in_specs=[VMEM] * 3 + [ANYWHERE] * (6 + batch),
        out_specs=(ANYWHERE,) + (VMEM,) * (5 + 2 * batch),
        scratch_shapes=[pltpu.VMEM((batch, group, blk, width), BF), pltpu.VMEM((seq, head), F32), pltpu.VMEM((head, width), F32),
                        pltpu.VMEM(w_o.shape, BF), pltpu.VMEM(x.shape, BF), pltpu.VMEM(x.shape, BF), pltpu.VMEM((blk, width), BF),
                        DMA((batch, 13)), DMA((batch, 13)), DMA((3,)), DMA((batch, 2)), DMA((3 + batch,)), DMA((batch,))]
        + [pltpu.VMEM((seq, head), BF)] * (3 + batch),
        cost_estimate=pl.CostEstimate(flops=80 * 10 ** 9, bytes_accessed=2 * batch * seq * width, transcendentals=seq * seq),
        compiler_params=pltpu.CompilerParams(vmem_limit_bytes=63 * 1024 * 1024, collective_id=cid, has_side_effects=True),
        name='second',
    )(tok, w_post[None, :], lse, w_o, x, dy, q, k, v, *outs)
    return res[0], res[1][0], res[2:6], res[6:6 + batch], res[6 + batch:]


def bwd_start(*accs):
    for acc in accs:
        acc[...] = jnp.zeros_like(acc)


def bwd_blocks(first, last, q_ref, k_ref, v_ref, do_ref, lse_ref, dl_ref, dq_acc, dk_ref, dv_ref):
    seq, head = q_ref.shape
    scale = head ** -0.5
    wide = 2 * BWD_BLK
    ahead = lax.broadcasted_iota(jnp.int32, (BWD_BLK, wide), 1) - lax.broadcasted_iota(jnp.int32, (BWD_BLK, wide), 0)

    @pl.loop(first, last)
    def _(j):
        cols = block_of(j, BWD_BLK)
        k = k_ref[cols, :]
        v = v_ref[cols, :]

        def step(i, masked):
            rows = block_of(i, wide)
            q = q_ref[rows, :]
            do = do_ref[rows, :]
            st = nt(k, q) * scale
            if masked:
                st = jnp.where(ahead >= lax.rem(j, 2) * BWD_BLK, st, NEG_BIG)
            pt = jnp.exp(st - lse_ref[0:1, rows])
            dpt = nt(v, do)
            dst = (pt * (dpt - dl_ref[0:1, rows]) * scale).astype(BF)
            dv_ref[cols, :] += nn(pt.astype(BF), do)
            dk_ref[cols, :] += nn(dst, q)
            dq_acc[rows, :] += tn(dst, k)

        step(j // 2, True)

        @pl.loop(j // 2 + 1, seq // wide)
        def _(i):
            step(i, False)


def bwd_kernel(q_ref, k_ref, v_ref, do_ref, lse_ref, dl_ref, dq_ref, dk_ref, dv_ref, dq_acc):
    bwd_start(dq_acc, dk_ref, dv_ref)
    bwd_blocks(0, q_ref.shape[0] // BWD_BLK, q_ref, k_ref, v_ref, do_ref, lse_ref, dl_ref, dq_acc, dk_ref, dv_ref)
    dq_ref[...] = dq_acc[...].astype(BF)


def attn_bwd(q, k, v, do, lse, delta):
    seq, head = q.shape
    blk = BWD_BLK
    pairs = seq * (seq + blk) // 2
    return pl.pallas_call(
        bwd_kernel,
        out_shape=(jax.ShapeDtypeStruct((seq, head), BF), jax.ShapeDtypeStruct((seq, head), F32), jax.ShapeDtypeStruct((seq, head), F32)),
        in_specs=[pl.BlockSpec(memory_space=pltpu.VMEM)] * 6,
        out_specs=(pl.BlockSpec(memory_space=pltpu.VMEM),) * 3,
        scratch_shapes=[pltpu.VMEM((seq, head), F32)],
        cost_estimate=pl.CostEstimate(flops=10 * pairs * head, bytes_accessed=20 * seq * head, transcendentals=pairs),
        compiler_params=pltpu.CompilerParams(vmem_limit_bytes=32 * 1024 * 1024),
        name='attn_bwd',
    )(q, k, v, do, lse, delta)


def move_kernel(*refs):
    for src, dst in zip(refs[:len(refs) // 2], refs[len(refs) // 2:]):
        dst[...] = src[...].reshape(dst.shape)


def move(grid, out_shapes, in_specs, out_specs, operands):
    size = sum(s.size for s in out_shapes)
    return pl.pallas_call(
        move_kernel,
        grid=grid,
        out_shape=out_shapes,
        in_specs=in_specs,
        out_specs=out_specs,
        cost_estimate=pl.CostEstimate(flops=20 * size, bytes_accessed=4 * size, transcendentals=0),
        compiler_params=pltpu.CompilerParams(vmem_limit_bytes=32 * 1024 * 1024),
    )(*operands)


def spread_q(parts):
    group, rows, head = parts.shape
    return move((group,), (jax.ShapeDtypeStruct((rows, group * head), BF),),
                [pl.BlockSpec((1, rows, head), lambda c: (c, 0, 0))], (pl.BlockSpec((rows, head), lambda c: (0, c)),), (parts,))[0]


def spread_kv(parts):
    group, rows, head = parts.shape
    shape = jax.ShapeDtypeStruct((rows, group // 2 * head), BF)
    out = pl.BlockSpec((rows, head), lambda c: (0, c))
    return move((group // 2,), (shape, shape),
                [pl.BlockSpec((1, rows, head), lambda c: (2 * c, 0, 0)), pl.BlockSpec((1, rows, head), lambda c: (2 * c + 1, 0, 0))], (out, out), (parts, parts))


def place(whole):
    rows, wide = whole.shape
    spec = pl.BlockSpec((rows // 8, wide), lambda r: (r, 0))
    return move((8,), (jax.ShapeDtypeStruct((rows, wide), BF),), [spec], (spec,), (whole,))[0]


def solution(mesh):
    group = mesh.shape['sp']

    def device_step(x_in, dy_in, positions, w_q, w_k, w_v, w_o, w_pre, w_post, q_norm, k_norm):
        batch, seq_loc, width = x_in.shape
        head = q_norm.shape[0]
        heads = w_q.shape[1] // head
        kv_heads = w_k.shape[1] // head
        rep = group // kv_heads
        assert heads == group and rep == 2
        me = lax.axis_index('sp')
        even = (me % rep) == 0
        swap = [(d, d ^ 1) for d in range(group)]
        inv_freq = ROPE_BASE ** (-jnp.arange(head // 2, dtype=F32) * 2.0 / head)
        a_both, cosines, sines, tok, per = first(
            x_in, positions.astype(F32)[None, :], inv_freq[None, :], w_pre, q_norm, k_norm, w_q, w_k, w_v, group, 0)
        roper = functools.partial(norm_rope, cosines=cosines, sines=sines)

        y_out, dw_post, (dw_o, dq0, dk0, dv0), d_os, deltas = second(
            tok, w_o, x_in, dy_in, w_post, *per[0][:3], per[0][6], [p[5] for p in per], group, 1)
        dw_o_all = lax.all_gather(dw_o, 'sp', axis=0, tiled=True)

        d_mine, dqkv_tok = [], []
        dq_norm = dk_norm = 0.0
        for b in range(batch):
            q_rot, k_rot, v_raw, q_raw, k_raw, _, lse = per[b]
            if b == 0:
                dq_rot, dk_part, dv_part = dq0, dk0, dv0
            else:
                lse, _ = lax.optimization_barrier((lse, d_mine[b - 1]))
                dq_rot, dk_part, dv_part = attn_bwd(q_rot, k_rot, v_raw, d_os[b], lse, deltas[b])
            other = lax.ppermute(jnp.where(even, dv_part, dk_part), 'sp', swap)
            dkv = (jnp.where(even, dk_part, dv_part) + other).astype(BF)
            _, q_pull = jax.vjp(roper, q_raw, q_norm)
            _, k_pull = jax.vjp(roper, k_raw, k_norm)
            dq_proj, dqn = q_pull(dq_rot)
            dk_proj, dkn = k_pull(dkv)
            dq_norm = dq_norm + dqn
            dk_norm = dk_norm + jnp.where(even, dkn, 0.0)
            d_two = jnp.concatenate([dq_proj, jnp.where(even, dk_proj, dkv)], axis=1)
            d_mine.append(d_two)
            if b:
                d_two, dqkv_tok[b - 1] = lax.optimization_barrier((d_two, dqkv_tok[b - 1]))
            dqkv_tok.append(lax.all_to_all(d_two, 'sp', 0, 1, tiled=True))

        dw_q_part = sum(tn(a_both[b], d_mine[b][:, :head]) for b in range(batch)).astype(BF)
        dw_q_parts = lax.all_gather(dw_q_part, 'sp', axis=0, tiled=False)
        dw_kv_part = sum(tn(a_both[b], d_mine[b][:, head:]) for b in range(batch)).astype(BF)
        dw_kv_parts = lax.all_gather(dw_kv_part, 'sp', axis=0, tiled=False)
        dw_o_all = place(dw_o_all)
        dqkv_tok[1], dw_o_all = lax.optimization_barrier((dqkv_tok[1], dw_o_all))

        d_tok = jnp.concatenate(dqkv_tok, axis=0)
        d_tok = [d_tok[:, j * head:(j + 1) * head] for j in range(2 * group)]
        d_normed = (nt(jnp.concatenate(d_tok[0::2], axis=1), w_q)
                    + nt(jnp.concatenate(d_tok[1::4], axis=1), w_k)
                    + nt(jnp.concatenate(d_tok[3::4], axis=1), w_v)).astype(BF).reshape(batch, seq_loc, width)
        _, pre_pull = jax.vjp(pre_norm, x_in.astype(F32), w_pre)
        dx_norm, dw_pre = pre_pull(d_normed)
        dx_out = (dy_in.astype(F32) + dx_norm).astype(BF)
        dw_q_all = spread_q(dw_q_parts)
        dw_k_all, dw_v_all = spread_kv(dw_kv_parts)
        small = lax.psum((dw_pre, dw_post, dq_norm, dk_norm), 'sp')
        return (y_out, dx_out, dw_q_all, dw_k_all, dw_v_all, dw_o_all) + small

    token_spec = P('dp', 'sp', None)
    return jax.shard_map(device_step, mesh=mesh,
                         in_specs=(token_spec, token_spec, P(('dp', 'sp')), P(None, None), P(None, None), P(None, None), P(None, None), P(None), P(None), P(None), P(None)),
                         out_specs=(token_spec, token_spec, P('dp', None), P('dp', None), P('dp', None), P('dp', None), P('dp'), P('dp'), P('dp'), P('dp')),
                         check_vma=False)
```

```python
import functools
import math
import jax
import jax.numpy as jnp
from jax import lax
from jax.experimental import pallas as pl
from jax.experimental.pallas import tpu as pltpu
from jax.sharding import PartitionSpec as P

EPS = 1e-6
ROPE_BASE = 1000000.0
ROPE_SCALE = 8.0
NEG_BIG = -1e30
HALF_PI = (1.5625, 0.0081787109375, 0.00011730194091796875, 3.129243850708008e-07, 9.920935796805404e-10)
BWD_BLK = 256
MIB = 1024 * 1024
SENDS = 13
BF = jnp.bfloat16
F32 = jnp.float32
MESH = pl.DeviceIdType.MESH


def lane_mean(x):
    return jnp.mean(x, axis=-1, keepdims=True)


def rms_scale(x_f32, weight):
    inv_rms = lax.rsqrt(lane_mean(x_f32 * x_f32) + EPS)
    return x_f32 * inv_rms * (1.0 + weight)


def norm_rope(head_bf, weight, cosines, sines):
    half_dim = head_bf.shape[-1] // 2
    normed = rms_scale(head_bf.astype(F32), weight)
    first = normed[..., :half_dim]
    second = normed[..., half_dim:]
    rotated = jnp.concatenate([first * cosines - second * sines, second * cosines + first * sines], axis=-1)
    return rotated.astype(BF)


def nt(lhs, rhs):
    return lax.dot_general(lhs, rhs, (((1,), (1,)), ((), ())), preferred_element_type=F32)


def nn(lhs, rhs):
    return lax.dot_general(lhs, rhs, (((1,), (0,)), ((), ())), preferred_element_type=F32)


def tn(lhs, rhs):
    return lax.dot_general(lhs, rhs, (((0,), (0,)), ((), ())), preferred_element_type=F32)


def others_barrier(group, me):
    barrier = pltpu.get_barrier_semaphore()
    for step in range(1, group):
        pl.semaphore_signal(barrier, inc=1, device_id={'sp': lax.rem(me + step, group)}, device_id_type=MESH)
    pl.semaphore_wait(barrier, group - 1)


def block_of(index, size):
    return pl.ds(pl.multiple_of(index * size, size), size)


def fold(x, op):
    out = x[:, :128]
    for c in range(1, x.shape[1] // 128):
        out = op(out, x[:, c * 128:(c + 1) * 128])
    return out


def diagonal(size):
    return lax.broadcasted_iota(jnp.int32, (size, size), 0) == lax.broadcasted_iota(jnp.int32, (size, size), 1)


def as_row(column):
    size = column.shape[0]
    return jnp.sum(jnp.where(diagonal(size), jnp.broadcast_to(column, (size, size)), 0.0), axis=0, keepdims=True)


def as_column(row):
    size = row.shape[1]
    return jnp.sum(jnp.where(diagonal(size), jnp.broadcast_to(row, (size, size)), 0.0), axis=1, keepdims=True)


class Attention:
    def __init__(self, group, me, b, q_ref, k_ref, v_ref, o_ref, lse_ref, tok_ref, s_scr, acc, send_sem, recv_sem):
        self.group, self.me, self.b = group, me, b
        self.refs = q_ref, k_ref, v_ref, o_ref, lse_ref, tok_ref, s_scr, acc
        self.sems = send_sem, recv_sem
        self.blk, self.head = acc.shape
        self.mine = block_of(me, self.head)

    def copy_to(self, step):
        o_ref, tok_ref = self.refs[3], self.refs[5]
        peer = lax.rem(self.me + step, self.group)
        return pltpu.make_async_remote_copy(
            src_ref=o_ref.at[block_of(peer, self.blk), :],
            dst_ref=tok_ref.at[pl.ds(self.b * self.blk, self.blk), self.mine],
            send_sem=self.sems[0].at[self.b, step],
            recv_sem=self.sems[1].at[self.b, step],
            device_id={'sp': peer},
            device_id_type=MESH,
        )

    def blocks(self, hook=None):
        q_ref, k_ref, v_ref, o_ref, lse_ref, _, s_scr, acc = self.refs
        blk, head = self.blk, self.head
        scale = head ** -0.5
        wide = 2 * blk
        ahead = lax.broadcasted_iota(jnp.int32, (blk, wide), 0) - lax.broadcasted_iota(jnp.int32, (blk, wide), 1)

        @pl.loop(0, self.group)
        def _(step):
            if hook is not None:
                pl.when(step == self.group // 2)(hook)
            i = lax.rem(self.me + step, self.group)
            rows = block_of(i, blk)
            q = q_ref[rows, :]
            edge = i // 2
            cols = block_of(edge, wide)
            s = jnp.where(ahead + lax.rem(i, 2) * blk >= 0, nt(q, k_ref[cols, :]) * scale, NEG_BIG)
            s_scr[:, cols] = s

            def pass1(j, m):
                cols = block_of(j, wide)
                s = nt(q, k_ref[cols, :]) * scale
                s_scr[:, cols] = s
                return jnp.maximum(m, fold(s, jnp.maximum))

            m = lax.fori_loop(0, edge, pass1, fold(s, jnp.maximum))
            m = jnp.max(m, axis=1, keepdims=True)

            @pl.when(step > 1)
            def _():
                self.copy_to(step - 1).start()

            def pass2(j, l):
                cols = block_of(j, wide)
                p = jnp.exp(s_scr[:, cols] - m)
                s_scr[:, cols] = p
                return l + fold(p, jnp.add)

            l = lax.fori_loop(0, edge + 1, pass2, jnp.zeros((blk, min(128, blk)), F32))
            l = jnp.sum(l, axis=1, keepdims=True)
            inv = 1.0 / l
            acc[...] = jnp.zeros_like(acc)

            @pl.loop(0, edge + 1)
            def _(j):
                cols = block_of(j, wide)
                acc[...] += nn((s_scr[:, cols] * inv).astype(BF), v_ref[cols, :])

            o_ref[rows, :] = acc[...].astype(BF)
            lse_ref[:, rows] = as_row(m + jnp.log(l))

    def flush(self):
        o_ref, tok_ref = self.refs[3], self.refs[5]
        tok_ref[pl.ds(self.b * self.blk, self.blk), self.mine] = o_ref[block_of(self.me, self.blk), :]
        self.copy_to(self.group - 1).start()

    def finish(self):
        @pl.loop(1, self.group)
        def _(step):
            self.copy_to(step).wait()


RIGHT_0, RIGHT_1, RIGHT_F, LEFT_1, LEFT_0, LEFT_F, SIB, SIB_L0, SIB_L1, SIB_R0, SIB_R1, SIB_O0, SIB_O1 = range(13)


class Ring:
    def __init__(self, group, me, buf, send_sem, recv_sem):
        self.me, self.chips = me, group // 2
        self.core, self.chip = lax.rem(me, 2), me // 2
        self.buf, self.sems = buf, (send_sem, recv_sem)
        self.blk = buf.shape[2]
        self.right, self.left, self.far = self.device(1, 0), self.device(-1, 0), self.device(2, 0)
        self.plans = [self.plan(b) for b in range(buf.shape[0])]

    def device(self, chip_step, other):
        return 2 * lax.rem(self.chip + self.chips + chip_step, self.chips) + lax.rem(self.core + other, 2)

    def send(self, b, which, owner, rows, to):
        place = self.buf.at[b, owner, rows]
        return pltpu.make_async_remote_copy(
            src_ref=place,
            dst_ref=place,
            send_sem=self.sems[0].at[b, which],
            recv_sem=self.sems[1].at[b, which],
            device_id={'sp': to},
            device_id_type=MESH,
        )

    def plan(self, b):
        me, right, left, far, sib = self.me, self.right, self.left, self.far, self.device(0, 1)
        half = self.blk // 2
        halves = [pl.ds(0, half), pl.ds(half, half)]
        routes = ((RIGHT_0, me, 0, right), (RIGHT_1, me, 1, right), (LEFT_1, me, 1, left), (LEFT_0, me, 0, left),
                  (RIGHT_F, left, 0, right), (LEFT_F, right, 1, left), (SIB_L0, left, 0, sib), (SIB_L1, left, 1, sib),
                  (SIB_R0, right, 0, sib), (SIB_R1, right, 1, sib), (SIB_O0, far, 0, sib), (SIB_O1, far, 1, sib))
        table = {which: self.send(b, which, owner, halves[rows], to) for which, owner, rows, to in routes}
        table[SIB] = self.send(b, SIB, me, pl.ds(0, self.blk), sib)
        return table

    def go(self, b, *which):
        for w in which:
            self.plans[b][w].start()

    def got(self, b, *which):
        for w in which:
            self.plans[b][w].wait_recv()

    def open(self, b):
        self.go(b, RIGHT_0, LEFT_1, RIGHT_1, LEFT_0, SIB)

    def turn(self, b):
        self.got(b, RIGHT_0, LEFT_1)
        self.go(b, RIGHT_F, LEFT_F, SIB_L0, SIB_R1)

    def near(self, b):
        self.got(b, RIGHT_1, LEFT_0)
        self.go(b, SIB_L1, SIB_R0)

    def each(self, b, work, middle):
        @pl.loop(0, 2 * self.chips)
        def _(t):
            @pl.when(t == 0)
            def _():
                self.got(b, SIB)

            @pl.when(t == 2)
            def _():
                middle(b)
                self.near(b)
                self.got(b, SIB_L0, SIB_R1, SIB_L1, SIB_R0)

            @pl.when(t == 6)
            def _():
                self.got(b, RIGHT_F, LEFT_F)
                self.go(b, SIB_O0, SIB_O1)
                self.got(b, SIB_O0, SIB_O1)

            own, far = t < 2, t >= 6
            chip_step = jnp.where(own, 0, jnp.where(far, 2, 1 + 2 * lax.rem(t, 2)))
            other = jnp.where(own | far, lax.rem(t, 2), (t - 2) // 2)
            work(b, self.device(chip_step, other))

    def sent(self):
        for plan in self.plans:
            for copy in plan.values():
                copy.wait_send()


def table_block(pos_row, freq_row):
    angle = as_column(pos_row) / ROPE_SCALE * freq_row
    turn = jnp.floor(angle * (2.0 / math.pi) + 0.5)
    rest = angle
    for part in HALF_PI:
        rest = rest - turn * part
    sq = rest * rest
    sin_r = rest + rest * sq * (-1.6666654611e-1 + sq * (8.3321608736e-3 + sq * -1.9515295891e-4))
    cos_r = 1.0 - 0.5 * sq + sq * sq * (4.166664568298827e-2 + sq * (-1.388731625493765e-3 + sq * 2.443315711809948e-5))
    quarter = turn - 4.0 * jnp.floor(turn * 0.25)
    odd = (quarter == 1.0) | (quarter == 3.0)
    cosines = jnp.where(odd, sin_r, cos_r)
    sines = jnp.where(odd, cos_r, sin_r)
    cosines = jnp.where((quarter == 1.0) | (quarter == 2.0), -cosines, cosines)
    sines = jnp.where(quarter >= 2.0, -sines, sines)
    return cosines, sines


def first_kernel(group, batch, x_ref, pos_ref, freq_ref, wpre_ref, qn_ref, kn_ref, wq_ref, wk_ref, wv_ref, full_ref, cos_out, sin_out, tok_ref, *rest):
    per_out = [rest[:7], rest[7:12]]
    buf, w_ref, pos_all, s_scr, acc, cos_ref, sin_ref, o_send, o_recv, send_sem, recv_sem, out_sem, w_sem, p_send, p_recv, keep_sem, table_sem = rest[12:29]
    kept = rest[29:]
    per = [kept[:6] + (per_out[0][6],), kept[6:]]
    outward = [[pltpu.make_async_copy(per[b][n], per_out[b][n], keep_sem.at[b, n]) for n in range(6 - b)] for b in range(batch)]
    tables = [pltpu.make_async_copy(cos_ref, cos_out, table_sem.at[0]), pltpu.make_async_copy(sin_ref, sin_out, table_sem.at[1])]
    blk, _ = x_ref.shape[1:]
    head = qn_ref.shape[1]
    me = lax.axis_index('sp')
    loads = [pltpu.make_async_copy(ref.at[:, block_of(index, head)], w_ref.at[:, pl.ds(place * head, head)], w_sem.at[place])
             for place, (ref, index) in enumerate(((wq_ref, me), (wk_ref, me // 2), (wv_ref, me // 2)))]
    for load in loads:
        load.start()

    @pl.loop(0, batch * 4)
    def _(t):
        rows = block_of(lax.rem(t, 4), blk // 4)
        x = x_ref[t // 4, rows, :].astype(F32)
        inv = lax.rsqrt(lane_mean(x * x) + EPS)
        buf[t // 4, me, rows, :] = (x * inv * (1.0 + wpre_ref[...])).astype(BF)

    others_barrier(group, me)
    ring = Ring(group, me, buf, send_sem, recv_sem)

    def pos_copy(step):
        return pltpu.make_async_remote_copy(
            src_ref=pos_ref,
            dst_ref=pos_all.at[me],
            send_sem=p_send.at[step],
            recv_sem=p_recv.at[step],
            device_id={'sp': lax.rem(me + step, group)},
            device_id_type=MESH,
        )

    for step in range(1, group):
        pos_copy(step).start()

    def out_copy(b, owner):
        return pltpu.make_async_copy(buf.at[b, owner], full_ref.at[b, block_of(owner, blk), :], out_sem.at[b, owner])

    def norm_rope_block(raw, weight, cosines, sines):
        x = raw.astype(F32)
        normed = x * lax.rsqrt(lane_mean(x * x) + EPS) * (1.0 + weight)
        first, second = normed[:, :head // 2], normed[:, head // 2:]
        return jnp.concatenate([first * cosines - second * sines, second * cosines + first * sines], axis=1).astype(BF)

    def project(b, owner):
        q_ref, k_ref, v_ref, qw_ref, kw_ref = per[b][:5]
        out_copy(b, owner).start()
        rows = block_of(owner, blk)
        qkv = nn(buf[b, owner], w_ref[...]).astype(BF)
        cosines, sines = cos_ref[rows, :], sin_ref[rows, :]
        q_raw, k_raw = qkv[:, :head], qkv[:, head:2 * head]
        qw_ref[rows, :] = q_raw
        kw_ref[rows, :] = k_raw
        v_ref[rows, :] = qkv[:, 2 * head:]
        q_ref[rows, :] = norm_rope_block(q_raw, qn_ref[...], cosines, sines)
        k_ref[rows, :] = norm_rope_block(k_raw, kn_ref[...], cosines, sines)

    ring.open(0)
    pos_all[me] = pos_ref[...]
    for step in range(1, group):
        pos_copy(step).wait()

    @pl.loop(0, group)
    def _(owner):
        cosines, sines = table_block(pos_all[owner], freq_ref[...])
        cos_ref[block_of(owner, blk), :] = cosines
        sin_ref[block_of(owner, blk), :] = sines

    for copy in tables:
        copy.start()
    for load in loads:
        load.wait()
    attention = Attention(group, me, 0, *per[0][:3], *per[0][5:], tok_ref, s_scr, acc, o_send, o_recv)

    def middle(b):
        if b:
            attention.blocks(lambda: ring.turn(b))
            attention.flush()
            outward[0][5].start()
        else:
            ring.turn(b)
            ring.open(b + 1)

    for b in range(batch):
        ring.each(b, project, middle)
        for copy in outward[b][:5]:
            copy.start()
    attention.finish()
    ring.sent()
    for copy in tables + sum(outward, []):
        copy.wait()
    for b in range(batch):
        @pl.loop(0, group)
        def _(owner):
            out_copy(b, owner).wait()


VMEM = pl.BlockSpec(memory_space=pltpu.VMEM)
ANYWHERE = pl.BlockSpec(memory_space=pl.ANY)
DMA = pltpu.SemaphoreType.DMA


def first(x, pos, freq, w_pre, q_norm, k_norm, w_q, w_k, w_v, group, cid):
    batch, blk, width = x.shape
    head = q_norm.shape[0]
    seq = group * blk
    assert group == 8
    heads_out = jax.ShapeDtypeStruct((seq, head), BF)
    table = jax.ShapeDtypeStruct((seq, head // 2), F32)
    outs = pl.pallas_call(
        functools.partial(first_kernel, group, batch),
        out_shape=(jax.ShapeDtypeStruct((batch, seq, width), BF), table, table, jax.ShapeDtypeStruct((blk, group * head), BF))
        + (heads_out,) * 6 + (jax.ShapeDtypeStruct((1, seq), F32),) + (heads_out,) * 5,
        in_specs=[VMEM] * 6 + [ANYWHERE] * 3,
        out_specs=(ANYWHERE,) * 3 + (VMEM,) + (ANYWHERE,) * 6 + (VMEM,) + (ANYWHERE,) * 5,
        scratch_shapes=[pltpu.VMEM((batch, group, blk, width), BF), pltpu.VMEM((width, 3 * head), BF), pltpu.VMEM((group, 1, blk), F32),
                        pltpu.VMEM((blk, seq), F32), pltpu.VMEM((blk, head), F32), pltpu.VMEM((seq, head // 2), F32), pltpu.VMEM((seq, head // 2), F32),
                        DMA((1, group)), DMA((1, group)), DMA((batch, SENDS)), DMA((batch, SENDS)), DMA((batch, group)), DMA((3,)), DMA((group,)), DMA((group,)),
                        DMA((batch, 6)), DMA((2,))] + [pltpu.VMEM((seq, head), BF)] * 11,
        cost_estimate=pl.CostEstimate(flops=90 * 10 ** 9, bytes_accessed=2 * batch * seq * width, transcendentals=seq * seq),
        compiler_params=pltpu.CompilerParams(vmem_limit_bytes=62 * MIB, collective_id=cid, has_side_effects=True),
        name='first',
    )(x, pos, freq, w_pre[None, :], q_norm[None, :], k_norm[None, :], w_q, w_k, w_v)
    return outs[:4] + ((outs[4:11], outs[11:16]),)


def second_kernel(group, batch, tok_ref, wpost_ref, lse_ref, wo_hbm, x_hbm, dy_hbm, *rest):
    late_hbm, rest = rest[:7], rest[7:]
    lse1_ref, rest = rest[0], rest[1:]
    y_hbm, dwpost_ref, dwo_ref, dq_ref, dk_ref, dv_ref = rest[:6]
    do_refs, dl_refs, rest = rest[6:6 + batch], rest[6 + batch:6 + 2 * batch], rest[6 + 2 * batch:]
    buf, dq_acc, dwo_acc, wo_ref, x_ref, dy_ref, p_scr, send_sem, recv_sem, wo_sem, act_sem, late_sem, y_sem = rest[:13]
    tok1_ref, s_scr, acc, o_send, o_recv, o1_ref = rest[13:19]
    late = rest[19:]
    q1_ref, k1_ref, v1_ref, q_ref, k_ref, v_ref, o0_ref = late
    o_refs = (o0_ref, o1_ref)
    toks = (tok_ref, tok1_ref)
    blk, width = x_ref.shape[1:]
    head = dwo_ref.shape[0]
    me = lax.axis_index('sp')
    mine = block_of(me, head)
    part = width // wo_sem.shape[0]

    def wo_load(n):
        cols = block_of(n, part)
        return pltpu.make_async_copy(wo_hbm.at[:, cols], wo_ref.at[:, cols], wo_sem.at[n])

    wo_loads = [wo_load(n) for n in range(width // part)]
    act_loads = [[pltpu.make_async_copy(src.at[b], dst.at[b], act_sem.at[b, n]) for n, (src, dst) in enumerate(((x_hbm, x_ref), (dy_hbm, dy_ref)))] for b in range(batch)]
    late_loads = [pltpu.make_async_copy(src, dst, late_sem.at[n]) for n, (src, dst) in enumerate(zip(late_hbm, late))]
    for load in wo_loads + sum(act_loads, []) + late_loads:
        load.start()
    dwpost_ref[...] = jnp.zeros_like(dwpost_ref)
    dwo_acc[...] = jnp.zeros_like(dwo_acc)
    y_copies = [pltpu.make_async_copy(x_ref.at[b], y_hbm.at[b], y_sem.at[b]) for b in range(batch)]

    def project(b):
        @pl.loop(0, width // part)
        def _(n):
            if b == 0:
                wo_load(n).wait()
            cols = block_of(n, part)
            p_scr[:, cols] = nn(toks[b][...], wo_ref[:, cols]).astype(BF)

        for load in act_loads[b]:
            load.wait()
        gain = 1.0 + wpost_ref[...]
        rows_each = 32

        @pl.loop(0, blk // rows_each)
        def _(t):
            rows = block_of(t, rows_each)
            p = p_scr[rows, :].astype(F32)
            dy = dy_ref[b, rows, :].astype(F32)
            inv = lax.rsqrt(lane_mean(p * p) + EPS)
            unit = p * inv
            x_ref[b, rows, :] = (x_ref[b, rows, :].astype(F32) + unit * gain).astype(BF)
            scaled = dy * gain
            dwpost_ref[...] += jnp.sum(dy * unit, axis=0, keepdims=True)
            buf[b, me, rows, :] = (inv * (scaled - unit * lane_mean(scaled * unit))).astype(BF)

        y_copies[b].start()

    project(0)
    others_barrier(group, me)
    ring = Ring(group, me, buf, send_sem, recv_sem)

    def work(b, owner):
        rows = block_of(owner, blk)
        chunk = buf[b, owner]
        o = o_refs[b][rows, :]
        d_o = nt(chunk, wo_ref[mine, :]).astype(BF)
        do_refs[b][rows, :] = d_o
        dl_refs[b][:, rows] = as_row(jnp.sum(d_o.astype(F32) * o.astype(F32), axis=1, keepdims=True))
        dwo_acc[...] += tn(o, chunk)

    def backward(hook):
        bwd_blocks(0, group, 3, hook, q_ref, k_ref, v_ref, do_refs[0], lse_ref, dl_refs[0], dq_acc, dk_ref, dv_ref)

    ring.open(0)
    for load in late_loads:
        load.wait()
    attention = Attention(group, me, 0, q1_ref, k1_ref, v1_ref, o1_ref, lse1_ref, tok1_ref, s_scr, acc, o_send, o_recv)
    attention.blocks()
    attention.flush()
    ring.turn(0)
    attention.finish()
    project(1)
    ring.open(1)

    def middle(b):
        if b:
            bwd_start(dq_acc, dk_ref, dv_ref)
            backward(lambda: ring.turn(b))
            dq_ref[...] = dq_acc[...].astype(BF)

    for b in range(batch):
        ring.each(b, work, middle)
    dwo_ref[...] = dwo_acc[...].astype(BF)
    ring.sent()
    for copy in y_copies:
        copy.wait()


def second(tok, w_o, x, dy, w_post, lse, late, group, cid):
    batch, blk, width = x.shape
    seq, head = late[0].shape
    assert batch == 2 and group == 8
    wide = jax.ShapeDtypeStruct((seq, head), F32)
    half = jax.ShapeDtypeStruct((seq, head), BF)
    row = jax.ShapeDtypeStruct((1, seq), F32)
    res = pl.pallas_call(
        functools.partial(second_kernel, group, batch),
        out_shape=(row, jax.ShapeDtypeStruct(x.shape, BF), jax.ShapeDtypeStruct((1, width), F32), jax.ShapeDtypeStruct((head, width), BF), half, wide, wide)
        + (half,) * batch + (row,) * batch,
        in_specs=[VMEM] * 3 + [ANYWHERE] * 10,
        out_specs=(VMEM, ANYWHERE) + (VMEM,) * (5 + 2 * batch),
        scratch_shapes=[pltpu.VMEM((batch, group, blk, width), BF), pltpu.VMEM((seq, head), F32), pltpu.VMEM((head, width), F32),
                        pltpu.VMEM(w_o.shape, BF), pltpu.VMEM(x.shape, BF), pltpu.VMEM(x.shape, BF), pltpu.VMEM((blk, width), BF),
                        DMA((batch, SENDS)), DMA((batch, SENDS)), DMA((3,)), DMA((batch, 2)), DMA((7,)), DMA((batch,)),
                        pltpu.VMEM(tok.shape, BF), pltpu.VMEM((blk, seq), F32), pltpu.VMEM((blk, head), F32), DMA((1, group)), DMA((1, group))]
        + [pltpu.VMEM((seq, head), BF)] * 8,
        cost_estimate=pl.CostEstimate(flops=80 * 10 ** 9, bytes_accessed=2 * batch * seq * width, transcendentals=seq * seq),
        compiler_params=pltpu.CompilerParams(vmem_limit_bytes=63 * MIB, collective_id=cid, has_side_effects=True),
        name='second',
    )(tok, w_post[None, :], lse, w_o, x, dy, *late)
    return res[0], res[1], res[2][0], res[3:7], res[7:7 + batch], res[7 + batch:]


def bwd_start(*accs):
    for acc in accs:
        acc[...] = jnp.zeros_like(acc)


def bwd_blocks(first, last, hook_at, hook, q_ref, k_ref, v_ref, do_ref, lse_ref, dl_ref, dq_acc, dk_ref, dv_ref):
    seq, head = q_ref.shape
    scale = head ** -0.5
    wide = 2 * BWD_BLK
    ahead = lax.broadcasted_iota(jnp.int32, (BWD_BLK, wide), 1) - lax.broadcasted_iota(jnp.int32, (BWD_BLK, wide), 0)

    @pl.loop(first, last)
    def _(j):
        if hook is not None:
            pl.when(j == hook_at)(hook)
        cols = block_of(j, BWD_BLK)
        k = k_ref[cols, :]
        v = v_ref[cols, :]

        def step(i, masked):
            rows = block_of(i, wide)
            q = q_ref[rows, :]
            do = do_ref[rows, :]
            st = nt(k, q) * scale
            if masked:
                st = jnp.where(ahead >= lax.rem(j, 2) * BWD_BLK, st, NEG_BIG)
            pt = jnp.exp(st - lse_ref[0:1, rows])
            dpt = nt(v, do)
            dst = (pt * (dpt - dl_ref[0:1, rows]) * scale).astype(BF)
            dv_ref[cols, :] += nn(pt.astype(BF), do)
            dk_ref[cols, :] += nn(dst, q)
            dq_acc[rows, :] += tn(dst, k)

        step(j // 2, True)

        @pl.loop(j // 2 + 1, seq // wide)
        def _(i):
            step(i, False)


def bwd_kernel(q_ref, k_ref, v_ref, do_ref, lse_ref, dl_ref, dq_ref, dk_ref, dv_ref, dq_acc):
    bwd_start(dq_acc, dk_ref, dv_ref)
    bwd_blocks(0, q_ref.shape[0] // BWD_BLK, 0, None, q_ref, k_ref, v_ref, do_ref, lse_ref, dl_ref, dq_acc, dk_ref, dv_ref)
    dq_ref[...] = dq_acc[...].astype(BF)


def attn_bwd(q, k, v, do, lse, delta):
    seq, head = q.shape
    blk = BWD_BLK
    pairs = seq * (seq + blk) // 2
    return pl.pallas_call(
        bwd_kernel,
        out_shape=(jax.ShapeDtypeStruct((seq, head), BF), jax.ShapeDtypeStruct((seq, head), F32), jax.ShapeDtypeStruct((seq, head), F32)),
        in_specs=[pl.BlockSpec(memory_space=pltpu.VMEM)] * 6,
        out_specs=(pl.BlockSpec(memory_space=pltpu.VMEM),) * 3,
        scratch_shapes=[pltpu.VMEM((seq, head), F32)],
        cost_estimate=pl.CostEstimate(flops=10 * pairs * head, bytes_accessed=20 * seq * head, transcendentals=pairs),
        compiler_params=pltpu.CompilerParams(vmem_limit_bytes=32 * MIB),
        name='attn_bwd',
    )(q, k, v, do, lse, delta)


def dw_kernel(d0_ref, d1_ref, a_hbm, out_ref, acc, a_buf, a_sem):
    seq, pair = d0_ref.shape
    width = a_buf.shape[2]
    head = pair // 2
    chunk = a_buf.shape[1]
    per_seq = seq // chunk

    def a_load(n):
        return pltpu.make_async_copy(a_hbm.at[n // per_seq, block_of(lax.rem(n, per_seq), chunk), :], a_buf.at[lax.rem(n, 2)], a_sem.at[lax.rem(n, 2)])

    a_load(0).start()
    acc[...] = jnp.zeros_like(acc)

    @pl.loop(0, 2 * per_seq)
    def _(n):
        @pl.when(n + 1 < 2 * per_seq)
        def _():
            a_load(n + 1).start()

        a_load(n).wait()
        rows = block_of(lax.rem(n, per_seq), chunk)

        def add(d_ref):
            @pl.loop(0, 2)
            def _(h):
                part = block_of(h, head)
                acc[part, :] += tn(d_ref[rows, part], a_buf[lax.rem(n, 2)])

        pl.when(n < per_seq)(lambda: add(d0_ref))
        pl.when(n >= per_seq)(lambda: add(d1_ref))

    @pl.loop(0, width // head)
    def _(r):
        cols = block_of(r, head)
        out_ref[cols, :] = acc[:, cols].T.astype(BF)


def weight_grad(d_mine, a_both):
    seq, pair = d_mine[0].shape
    width = a_both.shape[2]
    return pl.pallas_call(
        dw_kernel,
        out_shape=jax.ShapeDtypeStruct((width, pair), BF),
        in_specs=[VMEM, VMEM, ANYWHERE],
        out_specs=VMEM,
        scratch_shapes=[pltpu.VMEM((pair, width), F32), pltpu.VMEM((2, 512, width), BF), DMA((2,))],
        cost_estimate=pl.CostEstimate(flops=4 * seq * pair * width, bytes_accessed=4 * seq * width, transcendentals=0),
        compiler_params=pltpu.CompilerParams(vmem_limit_bytes=48 * MIB),
        name='weight_grad',
    )(*d_mine, a_both)


def dx_kernel(t0_ref, t1_ref, x_ref, dy_ref, wpre_ref, wq_hbm, wk_hbm, wv_hbm, dx_ref, sum_ref, da, w_buf, w_sem):
    batch, blk, _ = x_ref.shape
    head = w_buf.shape[2] // 4
    chips = wk_hbm.shape[1] // head

    def w_loads(c):
        slot = lax.rem(c, 2)
        sources = (wq_hbm.at[:, block_of(2 * c, head)], wk_hbm.at[:, block_of(c, head)], wq_hbm.at[:, block_of(2 * c + 1, head)], wv_hbm.at[:, block_of(c, head)])
        return [pltpu.make_async_copy(src, w_buf.at[slot, :, pl.ds(n * head, head)], w_sem.at[slot, n]) for n, src in enumerate(sources)]

    for load in w_loads(0):
        load.start()
    da[...] = jnp.zeros_like(da)

    @pl.loop(0, chips)
    def _(c):
        @pl.when(c + 1 < chips)
        def _():
            for load in w_loads(c + 1):
                load.start()

        for load in w_loads(c):
            load.wait()
        for b, t_ref in enumerate((t0_ref, t1_ref)):
            da[b * blk:(b + 1) * blk, :] += nt(t_ref[:, block_of(c, 4 * head)], w_buf[lax.rem(c, 2)])

    gain = 1.0 + wpre_ref[...]
    rows_each = 32
    sum_ref[...] = jnp.zeros_like(sum_ref)

    @pl.loop(0, batch * blk // rows_each)
    def _(t):
        per_b = blk // rows_each
        rows = block_of(lax.rem(t, per_b), rows_each)
        x = x_ref[t // per_b, rows, :].astype(F32)
        d = da[block_of(t, rows_each), :].astype(BF).astype(F32)
        inv = lax.rsqrt(lane_mean(x * x) + EPS)
        unit = x * inv
        scaled = d * gain
        sum_ref[...] += jnp.sum(d * unit, axis=0, keepdims=True)
        dx_ref[t // per_b, rows, :] = (dy_ref[t // per_b, rows, :].astype(F32) + inv * (scaled - unit * lane_mean(scaled * unit))).astype(BF)


def input_grad(tokens, x, dy, w_pre, w_q, w_k, w_v, head):
    batch, blk, width = x.shape
    size = batch * blk * tokens[0].shape[1] * width
    return pl.pallas_call(
        dx_kernel,
        out_shape=(jax.ShapeDtypeStruct(x.shape, BF), jax.ShapeDtypeStruct((1, width), F32)),
        in_specs=[VMEM] * 5 + [ANYWHERE] * 3,
        out_specs=(VMEM, VMEM),
        scratch_shapes=[pltpu.VMEM((batch * blk, width), F32), pltpu.VMEM((2, width, 4 * head), BF), DMA((2, 4))],
        cost_estimate=pl.CostEstimate(flops=2 * size, bytes_accessed=4 * width * width, transcendentals=0),
        compiler_params=pltpu.CompilerParams(vmem_limit_bytes=48 * MIB),
        name='input_grad',
    )(*tokens, x, dy, w_pre[None, :], w_q, w_k, w_v)


def move_kernel(*refs):
    for src, dst in zip(refs[:len(refs) // 2], refs[len(refs) // 2:]):
        dst[...] = src[...].reshape(dst.shape)


def move(grid, out_shapes, in_specs, out_specs, operands):
    size = sum(s.size for s in out_shapes)
    return pl.pallas_call(
        move_kernel,
        grid=grid,
        out_shape=out_shapes,
        in_specs=in_specs,
        out_specs=out_specs,
        cost_estimate=pl.CostEstimate(flops=20 * size, bytes_accessed=4 * size, transcendentals=0),
        compiler_params=pltpu.CompilerParams(vmem_limit_bytes=60 * MIB),
    )(*operands)


def spread(parts):
    group, rows, pair = parts.shape
    head = pair // 2
    tile = rows // 2
    narrow = jax.ShapeDtypeStruct((rows, group // 2 * head), BF)

    def body(even, odd, q_out, k_out, v_out):
        q_out[:, :head] = even[0, :, :head]
        q_out[:, head:] = odd[0, :, :head]
        k_out[...] = even[0, :, head:]
        v_out[...] = odd[0, :, head:]

    thin = pl.BlockSpec((tile, head), lambda r, c: (r, c))
    return pl.pallas_call(
        body,
        grid=(2, group // 2),
        out_shape=(jax.ShapeDtypeStruct((rows, group * head), BF), narrow, narrow),
        in_specs=[pl.BlockSpec((1, tile, pair), lambda r, c: (2 * c, r, 0)), pl.BlockSpec((1, tile, pair), lambda r, c: (2 * c + 1, r, 0))],
        out_specs=(pl.BlockSpec((tile, 2 * head), lambda r, c: (r, c)), thin, thin),
        cost_estimate=pl.CostEstimate(flops=20 * parts.size, bytes_accessed=4 * parts.size, transcendentals=0),
        compiler_params=pltpu.CompilerParams(vmem_limit_bytes=60 * MIB),
        name='spread',
    )(parts, parts)


def place(whole):
    rows, wide = whole.shape
    spec = pl.BlockSpec((rows // 8, wide), lambda r: (r, 0))
    return move((8,), (jax.ShapeDtypeStruct((rows, wide), BF),), [spec], (spec,), (whole,))[0]


def solution(mesh):
    group = mesh.shape['sp']

    def device_step(x_in, dy_in, positions, w_q, w_k, w_v, w_o, w_pre, w_post, q_norm, k_norm):
        batch, _, _ = x_in.shape
        head = q_norm.shape[0]
        heads = w_q.shape[1] // head
        kv_heads = w_k.shape[1] // head
        rep = group // kv_heads
        assert heads == group and rep == 2
        me = lax.axis_index('sp')
        even = (me % rep) == 0
        swap = [(d, d ^ 1) for d in range(group)]
        inv_freq = ROPE_BASE ** (-jnp.arange(head // 2, dtype=F32) * 2.0 / head)
        a_both, cosines, sines, tok, per = first(
            x_in, positions.astype(F32)[None, :], inv_freq[None, :], w_pre, q_norm, k_norm, w_q, w_k, w_v, group, 0)
        roper = functools.partial(norm_rope, cosines=cosines, sines=sines)

        lse1, y_out, dw_post, (dw_o, dq0, dk0, dv0), d_os, deltas = second(
            tok, w_o, x_in, dy_in, w_post, per[0][6], (*per[1][:3], *per[0][:3], per[0][5]), group, 1)
        dw_o_all = lax.all_gather(dw_o, 'sp', axis=0, tiled=True)

        d_mine, dqkv_tok = [], []
        dq_norm = dk_norm = 0.0
        for b in range(batch):
            q_rot, k_rot, v_raw, q_raw, k_raw = per[b][:5]
            if b == 0:
                dq_rot, dk_part, dv_part = dq0, dk0, dv0
            else:
                lse, _ = lax.optimization_barrier((lse1, d_mine[b - 1]))
                dq_rot, dk_part, dv_part = attn_bwd(q_rot, k_rot, v_raw, d_os[b], lse, deltas[b])
            other = lax.ppermute(jnp.where(even, dv_part, dk_part), 'sp', swap)
            dkv = (jnp.where(even, dk_part, dv_part) + other).astype(BF)
            _, q_pull = jax.vjp(roper, q_raw, q_norm)
            _, k_pull = jax.vjp(roper, k_raw, k_norm)
            dq_proj, dqn = q_pull(dq_rot)
            dk_proj, dkn = k_pull(dkv)
            dq_norm = dq_norm + dqn
            dk_norm = dk_norm + jnp.where(even, dkn, 0.0)
            d_two = jnp.concatenate([dq_proj, jnp.where(even, dk_proj, dkv)], axis=1)
            d_mine.append(d_two)
            if b:
                d_two, dqkv_tok[b - 1] = lax.optimization_barrier((d_two, dqkv_tok[b - 1]))
            dqkv_tok.append(lax.all_to_all(d_two, 'sp', 0, 1, tiled=True))

        dw_all = lax.all_gather(weight_grad(d_mine, a_both), 'sp', axis=0, tiled=False)
        dw_o_all = place(dw_o_all)
        dqkv_tok[1], dw_o_all = lax.optimization_barrier((dqkv_tok[1], dw_o_all))
        dx_out, dw_pre = input_grad(dqkv_tok, x_in, dy_in, w_pre, w_q, w_k, w_v, head)
        dw_q_all, dw_k_all, dw_v_all = spread(dw_all)
        dw_pre = dw_pre[0]
        small = lax.psum((dw_pre, dw_post, dq_norm, dk_norm), 'sp')
        return (y_out, dx_out, dw_q_all, dw_k_all, dw_v_all, dw_o_all) + small

    token_spec = P('dp', 'sp', None)
    return jax.shard_map(device_step, mesh=mesh,
                         in_specs=(token_spec, token_spec, P(('dp', 'sp'))) + (P(None, None),) * 4 + (P(None),) * 4,
                         out_specs=(token_spec, token_spec) + (P('dp', None),) * 4 + (P('dp'),) * 4,
                         check_vma=False)
```
